8 devices in a mesh: dp: 1 (over z), fsdp: 2 (over y), ep: 4 (over x, core).
Axes of the slice: x: 2, y: 2, z: 1, core: 2. Of those that a mesh axis runs over, the one named last changes fastest.
Arguments:
- hidden: bfloat16 [16384, 2304], P(('dp', 'fsdp', 'ep'))
- norm_gain: bfloat16 [2304], replicated
- w_router: bfloat16 [2304, 8], replicated
- w_gate: bfloat16 [8, 2304, 5760], P('ep', 'fsdp')
- w_up: bfloat16 [8, 2304, 5760], P('ep', 'fsdp')
- w_down: bfloat16 [8, 5760, 2304], P('ep', None, 'fsdp')
- top2_ids: int32 [16384, 2], P(('dp', 'fsdp', 'ep'))
Outputs:
- output: bfloat16 [16384, 2304], P(('dp', 'fsdp', 'ep'))
All inputs are finite; a program needn't handle non-finite values.
Results may differ from the reference program's by a relative error of at most 0.001.
Values are sent between devices in bfloat16 or wider.
A program may use at most 1 GiB of HBM per device.

```python
import jax
import jax.numpy as jnp
import numpy as np
from jax import lax

D = 2304
FF = 5760
EXPERTS = 8
TOKENS_DEV = 2048
GROUPS = 8
TOKENS = GROUPS * TOKENS_DEV
CAPACITY = (5 * TOKENS_DEV + 2 * EXPERTS - 1) // (2 * EXPERTS)
EPS = 1e-5


def draw_routes(route_key):
    perm_key, first_key, second_key = jax.random.split(route_key, 3)
    hot_count = max(EXPERTS // 4, 1)
    route_table = jnp.asarray(np.repeat(np.arange(EXPERTS), np.where(np.arange(EXPERTS) < hot_count, 4, 1)), dtype=jnp.int32)
    expert_perm = jax.random.permutation(perm_key, EXPERTS)
    table_pick = jax.random.randint(first_key, (TOKENS,), 0, route_table.shape[0])
    local_index = jnp.arange(TOKENS, dtype=jnp.int32) % TOKENS_DEV
    first_choice = jnp.where(local_index < EXPERTS, local_index, expert_perm[route_table[table_pick]])
    second_shift = jax.random.randint(second_key, (TOKENS,), 1, EXPERTS)
    second_choice = (first_choice + second_shift) % EXPERTS
    return jnp.stack([first_choice, second_choice], axis=1).astype(jnp.int32)


def setup_inputs(seed: int = 0, part: int = 0) -> dict:
    part_key = jax.random.fold_in(jax.random.key(seed), part)
    hidden_key, route_key = jax.random.split(part_key, 2)
    gain_key, router_key, gate_key, up_key, down_key = jax.random.split(jax.random.key(seed + 1), 5)
    hidden = jax.random.normal(hidden_key, (TOKENS, D), jnp.float32)
    norm_gain = jax.random.uniform(gain_key, (D,), jnp.float32, 0.5, 1.5)
    w_router = jax.random.normal(router_key, (D, EXPERTS), jnp.float32) * (0.5 * D ** -0.5)
    w_gate = jax.random.normal(gate_key, (EXPERTS, D, FF), jnp.float32) * D ** -0.5
    w_up = jax.random.normal(up_key, (EXPERTS, D, FF), jnp.float32) * D ** -0.5
    w_down = jax.random.normal(down_key, (EXPERTS, FF, D), jnp.float32) * FF ** -0.5
    return {
        'hidden': hidden.astype(jnp.bfloat16),
        'norm_gain': norm_gain.astype(jnp.bfloat16),
        'w_router': w_router.astype(jnp.bfloat16),
        'w_gate': w_gate.astype(jnp.bfloat16),
        'w_up': w_up.astype(jnp.bfloat16),
        'w_down': w_down.astype(jnp.bfloat16),
        'top2_ids': draw_routes(route_key),
    }


def expert_ffn(expert_pack):
    rows_in, gate_mat, up_mat, down_mat = expert_pack
    act_a = jnp.dot(rows_in, gate_mat, preferred_element_type=jnp.float32)
    act_b = jnp.dot(rows_in, up_mat, preferred_element_type=jnp.float32)
    hidden_act = (jax.nn.silu(act_a) * act_b).astype(jnp.bfloat16)
    return jnp.dot(hidden_act, down_mat, preferred_element_type=jnp.float32).astype(jnp.bfloat16)


def reference(hidden, norm_gain, w_router, w_gate, w_up, w_down, top2_ids):
    hidden_f32 = hidden.astype(jnp.float32)
    mean_sq = jnp.mean(hidden_f32 * hidden_f32, axis=-1, keepdims=True)
    normed = (hidden_f32 * lax.rsqrt(mean_sq + EPS) * norm_gain.astype(jnp.float32)).astype(jnp.bfloat16)
    logits = jnp.dot(normed, w_router, preferred_element_type=jnp.float32)
    gate_probs = jax.nn.softmax(jnp.take_along_axis(logits, top2_ids, axis=1), axis=-1)
    flat_ids = top2_ids.reshape(GROUPS, 2 * TOKENS_DEV)
    onehot = (flat_ids[:, :, None] == jnp.arange(EXPERTS, dtype=jnp.int32)).astype(jnp.int32)
    position = jnp.sum((jnp.cumsum(onehot, axis=1) - 1) * onehot, axis=2)
    group_base = jnp.arange(GROUPS, dtype=jnp.int32)[:, None] * (EXPERTS * CAPACITY)
    all_slots = GROUPS * EXPERTS * CAPACITY
    slot_ids = jnp.where(position < CAPACITY, group_base + flat_ids * CAPACITY + position, all_slots).reshape(TOKENS, 2)
    token_index = jnp.broadcast_to(jnp.arange(TOKENS, dtype=jnp.int32)[:, None], (TOKENS, 2))
    source = jnp.full((all_slots,), TOKENS, dtype=jnp.int32).at[slot_ids.reshape(-1)].set(token_index.reshape(-1), mode='drop')
    buffers = jnp.take(normed, source, axis=0, mode='fill', fill_value=0)
    by_expert = buffers.reshape(GROUPS, EXPERTS, CAPACITY, D).transpose(1, 0, 2, 3).reshape(EXPERTS, GROUPS * CAPACITY, D)
    expert_out = lax.map(expert_ffn, (by_expert, w_gate, w_up, w_down))
    out_flat = expert_out.reshape(EXPERTS, GROUPS, CAPACITY, D).transpose(1, 0, 2, 3).reshape(all_slots, D)
    returned = jnp.take(out_flat, slot_ids, axis=0, mode='fill', fill_value=0)
    moe_sum = jnp.sum(gate_probs[:, :, None] * returned.astype(jnp.float32), axis=1)
    return (hidden_f32 + moe_sum).astype(jnp.bfloat16)
```

```python
import functools

import jax
import jax.numpy as jnp
from jax import lax
from jax.experimental import pallas as pl
from jax.experimental.pallas import tpu as pltpu
from jax.sharding import PartitionSpec as P

EPS = 1e-5
MESH = pl.DeviceIdType.MESH
ANY = pl.BlockSpec(memory_space=pl.ANY)
VMEM = pl.BlockSpec(memory_space=pltpu.VMEM)
F32 = jnp.float32
BF16 = jnp.bfloat16
FF_CHUNKS = 5
HALF_CHUNKS = 3


def routes(top2_ids, num_experts, capacity):
    tok = top2_ids.shape[0]
    place = (top2_ids % 2) * (num_experts // 2) + top2_ids // 2
    choice = place[:, :, None] == jnp.arange(num_experts, dtype=jnp.int32)
    chosen = jnp.any(choice, axis=1)
    step = jnp.arange(tok, dtype=jnp.int32)
    before = (step[:, None] > step[None, :]).astype(BF16)
    position = jnp.dot(before, chosen.astype(BF16), preferred_element_type=F32).astype(jnp.int32)
    kept = jnp.where(chosen & (position < capacity), position, -1)
    base = jnp.arange(num_experts, dtype=jnp.int32) * capacity
    flat = jnp.where(kept >= 0, kept + base, -1)
    slots = jnp.sum(jnp.where(choice, flat[:, None, :], 0), axis=2)
    return kept.T, slots


def moe_kernel(cap, hid, gain, wr, meta, rows, wg, wu, wd,
               out, u_own, u_oth, gate_in, up_in, down_in, x_send, x_all, h_all, o_all, back,
               rows_oth, probs, local_sem, w_send, w_recv, d_send, d_recv, u_send, u_recv, x_ssem, x_rsem, b_send, b_recv):
    tok, d_model = hid.shape
    half = d_model // 2
    ff = wg.shape[2]
    fc = ff // FF_CHUNKS
    dc = half // HALF_CHUNKS
    n_dev = 8
    f = lax.axis_index('fsdp')
    j = lax.axis_index('ep')
    me = f * 4 + j
    j_low, j_high = lax.rem(j, 2), lax.div(j, 2)

    def peer(r):
        pf = 1 - f if r // 4 else f
        pj = (1 - j_low if r & 1 else j_low) + 2 * (1 - j_high if r & 2 else j_high)
        return pf, pj

    def remote(src, dst, ssem, rsem, r):
        pf, pj = peer(r)
        return pltpu.make_async_remote_copy(src_ref=src, dst_ref=dst, send_sem=ssem, recv_sem=rsem,
                                            device_id={'fsdp': pf, 'ep': pj}, device_id_type=MESH)

    def gate_copy(c):
        return remote(wg.at[1 - f, :, pl.ds(c * fc, fc)], gate_in.at[c], w_send.at[0, c], w_recv.at[0, c], 4)

    def up_copy(c):
        return remote(wu.at[1 - f, :, pl.ds(c * fc, fc)], up_in.at[c], w_send.at[1, c], w_recv.at[1, c], 4)

    def down_copy(q):
        return remote(wd.at[1 - f, :, pl.ds(q * dc, dc)], down_in.at[q], d_send.at[q], d_recv.at[q], 4)

    def rows_copy():
        return remote(rows, rows_oth, u_send.at[0], u_recv.at[0], 4)

    def u_copy():
        return remote(u_own, u_oth, u_send.at[1], u_recv.at[1], 4)

    def x_copy(s, r):
        pf, pj = peer(r)
        owner = me if s == 0 else (1 - f) * 4 + j
        return remote(x_send.at[s, pj], x_all.at[pl.ds(owner * cap, cap)], x_ssem.at[s, r], x_rsem.at[s, r], r)

    def back_copy(chunk, r):
        pf, pj = peer(r)
        return remote(o_all.at[chunk, pl.ds((pf * 4 + pj) * cap, cap)], back.at[chunk, pl.ds(me * cap, cap)],
                      b_send.at[chunk, r], b_recv.at[chunk, r], r)

    barrier = pltpu.get_barrier_semaphore()
    for r in range(1, n_dev):
        pf, pj = peer(r)
        pl.semaphore_signal(barrier, inc=1, device_id={'fsdp': pf, 'ep': pj}, device_id_type=MESH)
    pl.semaphore_wait(barrier, n_dev - 1)

    rows_copy().start()
    gate_copy(0).start()
    up_copy(0).start()

    def dispatch(u_buf, x_buf, onehot):
        block = 128
        load = pltpu.make_async_copy(hid, x_buf.at[pl.ds(0, tok)], local_sem.at[0])
        load.start()
        load.wait()
        gain_row = gain[...].astype(F32)
        lane = lax.broadcasted_iota(jnp.int32, (block, 128), 1)

        @pl.loop(0, tok // block)
        def _(i):
            here = pl.ds(pl.multiple_of(i * block, block), block)
            x = x_buf[here, :].astype(F32)
            mean_sq = jnp.mean(x * x, axis=-1, keepdims=True)
            u = (x * lax.rsqrt(mean_sq + EPS) * gain_row).astype(BF16)
            u_buf[here, :] = u
            logits = jnp.dot(u, wr[...], preferred_element_type=F32)
            info = meta[here, :]
            l0 = jnp.sum(jnp.where(lane == info[:, 0:1], logits, 0.0), axis=1, keepdims=True)
            l1 = jnp.sum(jnp.where(lane == info[:, 1:2], logits, 0.0), axis=1, keepdims=True)
            top = jnp.maximum(l0, l1)
            e0, e1 = jnp.exp(l0 - top), jnp.exp(l1 - top)
            total = e0 + e1
            probs[here, :] = jnp.where(lane == 0, e0 / total, e1 / total)

        keep = pltpu.make_async_copy(u_buf, u_own, local_sem.at[0])
        keep.start()
        keep.wait()
        u_copy().start()
        for c in range(1, FF_CHUNKS):
            gate_copy(c).start()
            up_copy(c).start()
        for q in range(HALF_CHUNKS):
            down_copy(q).start()

        for s in range(2):
            row_ref = rows if s == 0 else rows_oth
            owner = me if s == 0 else (1 - f) * 4 + j
            if s == 1:
                rows_copy().wait_recv()
                u_copy().wait_recv()
                load = pltpu.make_async_copy(u_oth, u_buf, local_sem.at[0])
                load.start()
                load.wait()

            @pl.loop(0, 4)
            def _(p):
                row = row_ref[pl.ds(f * 4 + p, 1), :]
                slot = lax.broadcasted_iota(jnp.int32, (cap, tok), 0)
                onehot[...] = jnp.where(slot == row, 1.0, 0.0).astype(BF16)

                @pl.loop(0, d_model // 256)
                def _(n):
                    cols = pl.ds(pl.multiple_of(n * 256, 256), 256)
                    x_buf[pl.ds(pl.multiple_of(p * cap, cap), cap), cols] = jnp.dot(
                        onehot[...], u_buf[:, cols], preferred_element_type=F32).astype(BF16)

                done = x_buf.at[pl.ds(pl.multiple_of(p * cap, cap), cap)]

                @pl.when(p == j)
                def _():
                    pltpu.make_async_copy(done, x_all.at[pl.ds(owner * cap, cap)], local_sem.at[p]).start()

                @pl.when(p != j)
                def _():
                    pltpu.make_async_copy(done, x_send.at[s, p], local_sem.at[p]).start()

            for p in range(4):
                pltpu.make_async_copy(x_buf.at[pl.ds(p * cap, cap)], x_send.at[s, p], local_sem.at[p]).wait()
            for r in (1, 2, 3):
                x_copy(s, r).start()

    pl.run_scoped(dispatch, pltpu.VMEM((tok, d_model), BF16), pltpu.VMEM((4 * cap, d_model), BF16), pltpu.VMEM((cap, tok), BF16))

    for s in range(2):
        for r in (1, 2, 3):
            x_copy(s, r).wait_recv()

    bm = 512
    sub = 256
    n_rows = n_dev * cap

    @pl.loop(0, FF_CHUNKS)
    def _(c):
        gate_copy(c).wait_recv()
        up_copy(c).wait_recv()

        def body(x_own, x_oth, g_own, g_oth, p_own, p_oth, h_ref):
            @pl.loop(0, bm // sub)
            def _(i):
                here = pl.ds(pl.multiple_of(i * sub, sub), sub)
                lhs_own, lhs_oth = x_own[here, :], x_oth[here, :]
                a = jnp.dot(lhs_own, g_own[...], preferred_element_type=F32) + jnp.dot(lhs_oth, g_oth[...], preferred_element_type=F32)
                b = jnp.dot(lhs_own, p_own[...], preferred_element_type=F32) + jnp.dot(lhs_oth, p_oth[...], preferred_element_type=F32)
                h_ref[here, :] = (a * jax.nn.sigmoid(a) * b).astype(BF16)

        pltpu.emit_pipeline(
            body, grid=(n_rows // bm,),
            in_specs=[pl.BlockSpec((bm, half), lambda i: (i, f)), pl.BlockSpec((bm, half), lambda i: (i, 1 - f)),
                      pl.BlockSpec((half, fc), lambda i: (0, c)), pl.BlockSpec((half, fc), lambda i: (0, 0)),
                      pl.BlockSpec((half, fc), lambda i: (0, c)), pl.BlockSpec((half, fc), lambda i: (0, 0))],
            out_specs=[pl.BlockSpec((bm, fc), lambda i: (i, c))],
        )(x_all, x_all, wg.at[f], gate_in.at[c], wu.at[f], up_in.at[c], h_all)

    def project(h_ref, w_ref, o_ref):
        @pl.loop(0, bm // sub)
        def _(i):
            here = pl.ds(pl.multiple_of(i * sub, sub), sub)
            o_ref[here, :] = jnp.dot(h_ref[here, :], w_ref[...], preferred_element_type=F32).astype(BF16)

    for phase in range(2):
        @pl.loop(0, HALF_CHUNKS)
        def _(q):
            if phase == 0:
                weight, col, chunk = wd.at[f], q, f * HALF_CHUNKS + q
            else:
                down_copy(q).wait_recv()
                weight, col, chunk = down_in.at[q], 0, (1 - f) * HALF_CHUNKS + q
            pltpu.emit_pipeline(
                project, grid=(n_rows // bm,),
                in_specs=[pl.BlockSpec((bm, ff), lambda i: (i, 0)), pl.BlockSpec((ff, dc), lambda i: (0, col))],
                out_specs=[pl.BlockSpec((bm, dc), lambda i: (i, 0))],
            )(h_all, weight, o_all.at[chunk])
            for r in range(1, n_dev):
                back_copy(chunk, r).start()

    def combine(b_buf, h_buf, onehot):
        block = 256

        @pl.loop(0, HALF_CHUNKS)
        def _(q):
            for side in range(2):
                chunk = side * HALF_CHUNKS + q
                cols = pl.ds(pl.multiple_of(chunk * dc, 128), dc)
                pltpu.make_async_copy(hid.at[:, cols], h_buf.at[side], local_sem.at[side]).start()
                for r in range(1, n_dev):
                    back_copy(chunk, r).wait_recv()
                for r in range(n_dev):
                    pf, pj = peer(r)
                    seg = pl.ds((pf * 4 + pj) * cap, cap)
                    src = back if r else o_all
                    pltpu.make_async_copy(src.at[chunk, seg], b_buf.at[seg, pl.ds(side * dc, dc)], local_sem.at[2 + side * 8 + r]).start()
            for side in range(2):
                chunk = side * HALF_CHUNKS + q
                cols = pl.ds(pl.multiple_of(chunk * dc, 128), dc)
                pltpu.make_async_copy(hid.at[:, cols], h_buf.at[side], local_sem.at[side]).wait()
                for r in range(n_dev):
                    pf, pj = peer(r)
                    seg = pl.ds((pf * 4 + pj) * cap, cap)
                    src = back if r else o_all
                    pltpu.make_async_copy(src.at[chunk, seg], b_buf.at[seg, pl.ds(side * dc, dc)], local_sem.at[2 + side * 8 + r]).wait()

            @pl.loop(0, tok // block)
            def _(i):
                here = pl.ds(pl.multiple_of(i * block, block), block)
                slot = lax.broadcasted_iota(jnp.int32, (block, n_rows), 1)
                info = meta[here, :]
                onehot[0:block, :] = jnp.where(slot == info[:, 2:3], 1.0, 0.0).astype(BF16)
                onehot[block:2 * block, :] = jnp.where(slot == info[:, 3:4], 1.0, 0.0).astype(BF16)
                p = probs[here, :]
                p0, p1 = p[:, 0:1], p[:, 1:2]
                picked = jnp.dot(onehot[...], b_buf[...], preferred_element_type=F32)
                for side in range(2):
                    part = picked[:, side * dc:(side + 1) * dc]
                    h_buf[side, here, :] = (h_buf[side, here, :].astype(F32) + (p0 * part[:block] + p1 * part[block:])).astype(BF16)

            for side in range(2):
                cols = pl.ds(pl.multiple_of((side * HALF_CHUNKS + q) * dc, 128), dc)
                pltpu.make_async_copy(h_buf.at[side], out.at[:, cols], local_sem.at[side]).start()
            for side in range(2):
                cols = pl.ds(pl.multiple_of((side * HALF_CHUNKS + q) * dc, 128), dc)
                pltpu.make_async_copy(h_buf.at[side], out.at[:, cols], local_sem.at[side]).wait()

    pl.run_scoped(combine, pltpu.VMEM((n_rows, 2 * dc), BF16), pltpu.VMEM((2, tok, dc), BF16), pltpu.VMEM((512, n_rows), BF16))

    rows_copy().wait_send()
    u_copy().wait_send()
    for c in range(FF_CHUNKS):
        gate_copy(c).wait_send()
        up_copy(c).wait_send()
    for q in range(HALF_CHUNKS):
        down_copy(q).wait_send()
    for s in range(2):
        for r in (1, 2, 3):
            x_copy(s, r).wait_send()

    @pl.loop(0, 2 * HALF_CHUNKS)
    def _(chunk):
        for r in range(1, n_dev):
            back_copy(chunk, r).wait_send()


def local_block(hidden, norm_gain, w_router, w_gate, w_up, w_down, top2_ids):
    tok, d_model = hidden.shape
    num_experts = w_router.shape[1]
    half, ff = w_gate.shape[1:]
    cap = (5 * tok + 2 * num_experts - 1) // (2 * num_experts)
    rows, slots = routes(top2_ids, num_experts, cap)
    meta = jnp.concatenate([top2_ids, slots], axis=1)
    router = jnp.pad(w_router, ((0, 0), (0, 128 - num_experts)))
    fc, dc = ff // FF_CHUNKS, half // HALF_CHUNKS
    n_rows = num_experts * cap
    shape = lambda *s: jax.ShapeDtypeStruct(s, BF16)
    dma = pltpu.SemaphoreType.DMA
    results = pl.pallas_call(
        functools.partial(moe_kernel, cap),
        out_shape=[shape(tok, d_model), shape(tok, d_model), shape(tok, d_model),
                   shape(FF_CHUNKS, half, fc), shape(FF_CHUNKS, half, fc), shape(HALF_CHUNKS, ff, dc),
                   shape(2, 4, cap, d_model), shape(n_rows, d_model), shape(n_rows, ff),
                   shape(2 * HALF_CHUNKS, n_rows, dc), shape(2 * HALF_CHUNKS, n_rows, dc)],
        in_specs=[ANY, VMEM, VMEM, VMEM, VMEM, ANY, ANY, ANY],
        out_specs=[ANY] * 11,
        scratch_shapes=[
            pltpu.VMEM((num_experts, tok), jnp.int32), pltpu.VMEM((tok, 128), F32),
            dma((18,)), dma((2, FF_CHUNKS)), dma((2, FF_CHUNKS)), dma((HALF_CHUNKS,)), dma((HALF_CHUNKS,)),
            dma((2,)), dma((2,)), dma((2, 4)), dma((2, 4)),
            dma((2 * HALF_CHUNKS, 8)), dma((2 * HALF_CHUNKS, 8))],
        compiler_params=pltpu.CompilerParams(collective_id=0, has_side_effects=True, vmem_limit_bytes=62 * 1024 * 1024),
    )(hidden, norm_gain[None, :], router, meta, rows, w_gate, w_up, w_down)
    return results[0]


def solution(mesh):
    tok_spec = P(('dp', 'fsdp', 'ep'), None)
    in_specs = (tok_spec, P(None), P(None, None), P('ep', 'fsdp', None), P('ep', 'fsdp', None), P('ep', None, 'fsdp'), tok_spec)
    return jax.shard_map(local_block, mesh=mesh, in_specs=in_specs, out_specs=tok_spec, check_vma=False)
```

```python
import functools

import jax
import jax.numpy as jnp
from jax import lax
from jax.experimental import pallas as pl
from jax.experimental.pallas import tpu as pltpu
from jax.sharding import PartitionSpec as P

EPS = 1e-5
MESH = pl.DeviceIdType.MESH
ANY = pl.BlockSpec(memory_space=pl.ANY)
VMEM = pl.BlockSpec(memory_space=pltpu.VMEM)
F32 = jnp.float32
BF16 = jnp.bfloat16
FF_CHUNKS = 5
HALF_CHUNKS = 3
PIECE = 128
TOK = 128
WINDOW = TOK + 16


def moe_kernel(cap, hid, gain, wr, ids, wg, wu, wd,
               out, u_own, u_oth, gate_in, up_in, down_in, x_send, x_all, h_all, o_all, back,
               rows, rows_oth, meta, probs, wr_pad, base_v, base_s, local_sem, w_send, w_recv, d_send, d_recv, u_send, u_recv, x_ssem, x_rsem, b_send, b_recv):
    tok, d_model = hid.shape
    half = d_model // 2
    ff = wg.shape[2]
    fc = ff // FF_CHUNKS
    dc = half // HALF_CHUNKS
    n_dev = 8
    pieces = dc // PIECE
    n_rows = n_dev * cap
    f = lax.axis_index('fsdp')
    j = lax.axis_index('ep')
    me = f * 4 + j
    j_low, j_high = lax.rem(j, 2), lax.div(j, 2)

    def peer(r):
        pf = 1 - f if r // 4 else f
        pj = (1 - j_low if r & 1 else j_low) + 2 * (1 - j_high if r & 2 else j_high)
        return pf, pj

    def remote(src, dst, ssem, rsem, r):
        pf, pj = peer(r)
        return pltpu.make_async_remote_copy(src_ref=src, dst_ref=dst, send_sem=ssem, recv_sem=rsem,
                                            device_id={'fsdp': pf, 'ep': pj}, device_id_type=MESH)

    def gate_copy(c):
        return remote(wg.at[1 - f, :, pl.ds(c * fc, fc)], gate_in.at[c], w_send.at[0, c], w_recv.at[0, c], 4)

    def up_copy(c):
        return remote(wu.at[1 - f, :, pl.ds(c * fc, fc)], up_in.at[c], w_send.at[1, c], w_recv.at[1, c], 4)

    def down_copy(q):
        return remote(wd.at[1 - f, :, pl.ds(q * dc, dc)], down_in.at[q], d_send.at[q], d_recv.at[q], 4)

    def rows_copy():
        return remote(rows, rows_oth, u_send.at[0], u_recv.at[0], 4)

    def u_copy():
        return remote(u_own, u_oth, u_send.at[1], u_recv.at[1], 4)

    def x_copy(s, r):
        pf, pj = peer(r)
        owner = me if s == 0 else (1 - f) * 4 + j
        return remote(x_send.at[s, pj], x_all.at[pl.ds(owner * cap, cap)], x_ssem.at[s, r], x_rsem.at[s, r], r)

    def back_copy(chunk, k, r):
        pf, pj = peer(r)
        cols = pl.ds(pl.multiple_of(k * PIECE, PIECE), PIECE)
        return remote(o_all.at[chunk, pl.ds((pf * 4 + pj) * cap, cap), cols], back.at[chunk, pl.ds(me * cap, cap), cols],
                      b_send.at[chunk * pieces + k, r], b_recv.at[chunk * pieces + k, r], r)

    barrier = pltpu.get_barrier_semaphore()
    for r in range(1, n_dev):
        pf, pj = peer(r)
        pl.semaphore_signal(barrier, inc=1, device_id={'fsdp': pf, 'ep': pj}, device_id_type=MESH)
    pl.semaphore_wait(barrier, n_dev - 1)

    gate_copy(0).start()
    up_copy(0).start()

    wr_pad[...] = jnp.zeros_like(wr_pad)
    wr_pad[0:n_dev, :] = wr[...]
    tri = (lax.broadcasted_iota(jnp.int32, (TOK, TOK), 0) < lax.broadcasted_iota(jnp.int32, (TOK, TOK), 1)).astype(F32).astype(BF16)
    spot = lax.broadcasted_iota(jnp.int32, (n_dev, TOK), 0)
    column = lax.broadcasted_iota(jnp.int32, (n_dev, TOK), 1)
    line = lax.broadcasted_iota(jnp.int32, (TOK, TOK), 0)

    def route(blk, carry):
        count, bases = carry
        here = pl.ds(pl.multiple_of(blk * TOK, TOK), TOK)
        id0, id1 = ids[0:1, here], ids[1:2, here]
        place0 = lax.rem(id0, 2) * 4 + lax.div(id0, 2)
        place1 = lax.rem(id1, 2) * 4 + lax.div(id1, 2)
        chosen = (spot == place0) | (spot == place1)
        before = jnp.dot(jnp.where(chosen, 1.0, 0.0).astype(BF16), tri, preferred_element_type=F32)
        position = before.astype(jnp.int32) + count
        kept = jnp.where(chosen & (position < cap), position, -1)
        rows[:, here] = kept
        flat = jnp.where(kept >= 0, kept + spot * cap, -1)
        slot0 = jnp.sum(jnp.where(spot == place0, flat, 0), axis=0, keepdims=True)
        slot1 = jnp.sum(jnp.where(spot == place1, flat, 0), axis=0, keepdims=True)
        stacked = jnp.where(line == 0, id0, jnp.where(line == 1, id1, jnp.where(line == 2, slot0, slot1)))
        meta[here, :] = stacked.astype(F32).T.astype(jnp.int32)
        start = jnp.minimum(lax.div(count, 16), (cap - WINDOW) // 16)
        bases = jnp.where(column == blk, start + spot * (cap // 16), bases)
        return count + jnp.sum(jnp.where(chosen, 1, 0), axis=1, keepdims=True), bases

    bases = lax.fori_loop(0, tok // TOK, route, (jnp.zeros((n_dev, 1), jnp.int32), jnp.zeros((n_dev, TOK), jnp.int32)))[1]
    base_v[...] = bases

    def dispatch(u_buf, x_buf, onehot):
        block = 128
        load = pltpu.make_async_copy(hid, x_buf.at[pl.ds(0, tok)], local_sem.at[0])
        load.start()
        pltpu.make_async_copy(base_v, base_s, local_sem.at[1]).start()
        load.wait()
        pltpu.make_async_copy(base_v, base_s, local_sem.at[1]).wait()
        gain_row = gain[...].astype(F32)[None, :]
        lane = lax.broadcasted_iota(jnp.int32, (block, 128), 1)

        @pl.loop(0, tok // block)
        def _(i):
            here = pl.ds(pl.multiple_of(i * block, block), block)
            x = x_buf[here, :].astype(F32)
            mean_sq = jnp.mean(x * x, axis=-1, keepdims=True)
            u = (x * lax.rsqrt(mean_sq + EPS) * gain_row).astype(BF16)
            u_buf[here, :] = u
            logits = lax.dot_general(u, wr_pad[...], (((1,), (1,)), ((), ())), preferred_element_type=F32)
            info = meta[here, :]
            l0 = jnp.sum(jnp.where(lane == info[:, 0:1], logits, 0.0), axis=1, keepdims=True)
            l1 = jnp.sum(jnp.where(lane == info[:, 1:2], logits, 0.0), axis=1, keepdims=True)
            top = jnp.maximum(l0, l1)
            e0, e1 = jnp.exp(l0 - top), jnp.exp(l1 - top)
            total = e0 + e1
            probs[here, :] = jnp.where(lane == 0, e0 / total, e1 / total)

        keep = pltpu.make_async_copy(u_buf, u_own, local_sem.at[0])
        keep.start()
        keep.wait()
        rows_copy().start()
        u_copy().start()
        for c in range(1, FF_CHUNKS):
            gate_copy(c).start()
            up_copy(c).start()
        for q in range(HALF_CHUNKS):
            down_copy(q).start()

        for s in range(2):
            row_ref = rows if s == 0 else rows_oth
            owner = me if s == 0 else (1 - f) * 4 + j
            if s == 1:
                rows_copy().wait_recv()
                u_copy().wait_recv()
                load = pltpu.make_async_copy(u_oth, u_buf, local_sem.at[0])
                load.start()
                load.wait()

            @pl.loop(0, 4)
            def _(p):
                row = row_ref[pl.ds(f * 4 + p, 1), :]
                slot = lax.broadcasted_iota(jnp.int32, (cap, tok), 0)
                onehot[...] = jnp.where(slot == row, 1.0, 0.0).astype(BF16)

                @pl.loop(0, d_model // 256)
                def _(n):
                    cols = pl.ds(pl.multiple_of(n * 256, 256), 256)
                    x_buf[pl.ds(pl.multiple_of(p * cap, cap), cap), cols] = jnp.dot(
                        onehot[...], u_buf[:, cols], preferred_element_type=F32).astype(BF16)

                done = x_buf.at[pl.ds(pl.multiple_of(p * cap, cap), cap)]

                @pl.when(p == j)
                def _():
                    pltpu.make_async_copy(done, x_all.at[pl.ds(owner * cap, cap)], local_sem.at[p]).start()

                @pl.when(p != j)
                def _():
                    pltpu.make_async_copy(done, x_send.at[s, p], local_sem.at[p]).start()

            for p in range(4):
                pltpu.make_async_copy(x_buf.at[pl.ds(p * cap, cap)], x_send.at[s, p], local_sem.at[p]).wait()
            for r in (1, 2, 3):
                x_copy(s, r).start()

    pl.run_scoped(dispatch, pltpu.VMEM((tok, d_model), BF16), pltpu.VMEM((4 * cap, d_model), BF16), pltpu.VMEM((cap, tok), BF16))

    for s in range(2):
        for r in (1, 2, 3):
            x_copy(s, r).wait_recv()

    bm = 512
    sub = 256

    @pl.loop(0, FF_CHUNKS)
    def _(c):
        gate_copy(c).wait_recv()
        up_copy(c).wait_recv()

        def body(x_own, x_oth, g_own, g_oth, p_own, p_oth, h_ref):
            @pl.loop(0, bm // sub)
            def _(i):
                here = pl.ds(pl.multiple_of(i * sub, sub), sub)
                lhs_own, lhs_oth = x_own[here, :], x_oth[here, :]
                a = jnp.dot(lhs_own, g_own[...], preferred_element_type=F32) + jnp.dot(lhs_oth, g_oth[...], preferred_element_type=F32)
                b = jnp.dot(lhs_own, p_own[...], preferred_element_type=F32) + jnp.dot(lhs_oth, p_oth[...], preferred_element_type=F32)
                h_ref[here, :] = (a * jax.nn.sigmoid(a) * b).astype(BF16)

        pltpu.emit_pipeline(
            body, grid=(n_rows // bm,),
            in_specs=[pl.BlockSpec((bm, half), lambda i: (i, f)), pl.BlockSpec((bm, half), lambda i: (i, 1 - f)),
                      pl.BlockSpec((half, fc), lambda i: (0, c)), pl.BlockSpec((half, fc), lambda i: (0, 0)),
                      pl.BlockSpec((half, fc), lambda i: (0, c)), pl.BlockSpec((half, fc), lambda i: (0, 0))],
            out_specs=[pl.BlockSpec((bm, fc), lambda i: (i, c))],
        )(x_all, x_all, wg.at[f], gate_in.at[c], wu.at[f], up_in.at[c], h_all)

    def project(h_ref, w_ref, o_ref):
        @pl.loop(0, bm // sub)
        def _(i):
            here = pl.ds(pl.multiple_of(i * sub, sub), sub)
            o_ref[here, :] = jnp.dot(h_ref[here, :], w_ref[...], preferred_element_type=F32).astype(BF16)

    for phase in range(2):
        @pl.loop(0, HALF_CHUNKS)
        def _(q):
            if phase == 0:
                weight, col, chunk = wd.at[f], q, f * HALF_CHUNKS + q
            else:
                down_copy(q).wait_recv()
                weight, col, chunk = down_in.at[q], 0, (1 - f) * HALF_CHUNKS + q
            pltpu.emit_pipeline(
                project, grid=(n_rows // bm,),
                in_specs=[pl.BlockSpec((bm, ff), lambda i: (i, 0)), pl.BlockSpec((ff, dc), lambda i: (0, col))],
                out_specs=[pl.BlockSpec((bm, dc), lambda i: (i, 0))],
            )(h_all, weight, o_all.at[chunk])
            for k in range(pieces):
                for r in range(1, n_dev):
                    back_copy(chunk, k, r).start()

    def combine(b_buf, h_buf, picks, window):
        n_blocks = tok // TOK
        lane = lax.broadcasted_iota(jnp.int32, (1, n_dev * WINDOW), 1)

        @pl.loop(0, n_blocks)
        def _(i):
            shift = jnp.zeros_like(lane)
            for e in range(n_dev):
                shift = jnp.where(lane >= e * WINDOW, base_s[e, i] * 16 - e * WINDOW, shift)
            row = lane + shift
            info = meta[pl.ds(pl.multiple_of(i * TOK, TOK), TOK), :]
            for k in range(2):
                picks[i, k * TOK:(k + 1) * TOK, :] = jnp.where(row == info[:, 2 + k:3 + k], 1.0, 0.0).astype(BF16)

        @pl.loop(0, HALF_CHUNKS * pieces)
        def _(step):
            q, k = lax.div(step, pieces), lax.rem(step, pieces)
            piece = pl.ds(pl.multiple_of(k * PIECE, PIECE), PIECE)

            def cols(side):
                return pl.ds(pl.multiple_of((side * HALF_CHUNKS + q) * dc + k * PIECE, PIECE), PIECE)

            def loads(side):
                moves = [pltpu.make_async_copy(hid.at[:, cols(side)], h_buf.at[side], local_sem.at[side])]
                for r in range(n_dev):
                    pf, pj = peer(r)
                    seg = pl.ds((pf * 4 + pj) * cap, cap)
                    src = back if r else o_all
                    moves.append(pltpu.make_async_copy(src.at[side * HALF_CHUNKS + q, seg, piece], b_buf.at[seg, pl.ds(side * PIECE, PIECE)], local_sem.at[2 + side * 8 + r]))
                return moves

            def store(side):
                return pltpu.make_async_copy(h_buf.at[side], out.at[:, cols(side)], local_sem.at[side])

            for side in range(2):
                for r in range(1, n_dev):
                    back_copy(side * HALF_CHUNKS + q, k, r).wait_recv()
                for move in loads(side):
                    move.start()
            for side in range(2):
                for move in loads(side):
                    move.wait()

            @pl.loop(0, n_blocks)
            def _(i):
                here = pl.ds(pl.multiple_of(i * TOK, TOK), TOK)
                for e in range(n_dev):
                    window[e * WINDOW:(e + 1) * WINDOW, :] = b_buf[pl.ds(base_s[e, i] * 16, WINDOW), :]
                p = probs[here, :]
                p0, p1 = p[:, 0:1], p[:, 1:2]
                picked = jnp.dot(picks[i], window[...], preferred_element_type=F32)
                moe = p0 * picked[:TOK] + p1 * picked[TOK:]
                for side in range(2):
                    h_buf[side, here, :] = (h_buf[side, here, :].astype(F32) + moe[:, side * PIECE:(side + 1) * PIECE]).astype(BF16)

            for side in range(2):
                store(side).start()
            for side in range(2):
                store(side).wait()

    pl.run_scoped(combine, pltpu.VMEM((n_rows, 2 * PIECE), BF16), pltpu.VMEM((2, tok, PIECE), BF16),
                  pltpu.VMEM((tok // TOK, 2 * TOK, n_dev * WINDOW), BF16), pltpu.VMEM((n_dev * WINDOW, 2 * PIECE), BF16))

    rows_copy().wait_send()
    u_copy().wait_send()
    for c in range(FF_CHUNKS):
        gate_copy(c).wait_send()
        up_copy(c).wait_send()
    for q in range(HALF_CHUNKS):
        down_copy(q).wait_send()
    for s in range(2):
        for r in (1, 2, 3):
            x_copy(s, r).wait_send()

    @pl.loop(0, 2 * HALF_CHUNKS)
    def _(chunk):
        for k in range(pieces):
            for r in range(1, n_dev):
                back_copy(chunk, k, r).wait_send()


def local_block(hidden, norm_gain, w_router, w_gate, w_up, w_down, top2_ids):
    tok, d_model = hidden.shape
    num_experts = w_router.shape[1]
    half, ff = w_gate.shape[1:]
    cap = (5 * tok + 2 * num_experts - 1) // (2 * num_experts)
    fc, dc = ff // FF_CHUNKS, half // HALF_CHUNKS
    n_rows = num_experts * cap
    shape = lambda *s: jax.ShapeDtypeStruct(s, BF16)
    dma = pltpu.SemaphoreType.DMA
    results = pl.pallas_call(
        functools.partial(moe_kernel, cap),
        out_shape=[shape(tok, d_model), shape(tok, d_model), shape(tok, d_model),
                   shape(FF_CHUNKS, half, fc), shape(FF_CHUNKS, half, fc), shape(HALF_CHUNKS, ff, dc),
                   shape(2, 4, cap, d_model), shape(n_rows, d_model), shape(n_rows, ff),
                   shape(2 * HALF_CHUNKS, n_rows, dc), shape(2 * HALF_CHUNKS, n_rows, dc)],
        in_specs=[ANY, VMEM, VMEM, VMEM, ANY, ANY, ANY],
        out_specs=[ANY] * 11,
        scratch_shapes=[
            pltpu.VMEM((num_experts, tok), jnp.int32), pltpu.VMEM((num_experts, tok), jnp.int32),
            pltpu.VMEM((tok, 128), jnp.int32), pltpu.VMEM((tok, 128), F32), pltpu.VMEM((128, d_model), BF16),
            pltpu.VMEM((num_experts, TOK), jnp.int32), pltpu.SMEM((num_experts, TOK), jnp.int32),
            dma((18,)), dma((2, FF_CHUNKS)), dma((2, FF_CHUNKS)), dma((HALF_CHUNKS,)), dma((HALF_CHUNKS,)),
            dma((2,)), dma((2,)), dma((2, 4)), dma((2, 4)),
            dma((d_model // PIECE, 8)), dma((d_model // PIECE, 8))],
        compiler_params=pltpu.CompilerParams(collective_id=0, has_side_effects=True, vmem_limit_bytes=62 * 1024 * 1024),
    )(hidden, norm_gain, w_router.T, top2_ids.T, w_gate, w_up, w_down)
    return results[0]


def solution(mesh):
    tok_spec = P(('dp', 'fsdp', 'ep'), None)
    in_specs = (tok_spec, P(None), P(None, None), P('ep', 'fsdp', None), P('ep', 'fsdp', None), P('ep', None, 'fsdp'), tok_spec)
    return jax.shard_map(local_block, mesh=mesh, in_specs=in_specs, out_specs=tok_spec, check_vma=False)
```

```python
import functools

import jax
import jax.numpy as jnp
from jax import lax
from jax.experimental import pallas as pl
from jax.experimental.pallas import tpu as pltpu
from jax.sharding import PartitionSpec as P

EPS = 1e-5
MESH = pl.DeviceIdType.MESH
ANY = pl.BlockSpec(memory_space=pl.ANY)
VMEM = pl.BlockSpec(memory_space=pltpu.VMEM)
F32 = jnp.float32
BF16 = jnp.bfloat16
FF_CHUNKS = 5
HALF_CHUNKS = 3
PIECE = 128
TOK = 128
WINDOW = TOK + 16


def moe_kernel(cap, hid, gain, wr, ids, wg, wu, wd,
               out, hid_oth, gate_in, up_in, down_in, x_send, x_all, h_all, o_all, back, y_own, y_oth,
               rows, ids_oth, meta, probs, wr_pad, base_v, base_s, local_sem, w_send, w_recv, d_send, d_recv,
               u_send, u_recv, x_ssem, x_rsem, b_send, b_recv, y_send, y_recv):
    tok, d_model = hid.shape
    half = d_model // 2
    ff = wg.shape[2]
    fc = ff // FF_CHUNKS
    dc = half // HALF_CHUNKS
    n_dev = 8
    pieces = dc // PIECE
    n_rows = n_dev * cap
    chunks = 2 * HALF_CHUNKS
    n_blocks = tok // TOK
    f = lax.axis_index('fsdp')
    j = lax.axis_index('ep')
    me = f * 4 + j
    j_low, j_high = lax.rem(j, 2), lax.div(j, 2)

    def peer(r):
        pf = 1 - f if r // 4 else f
        pj = (1 - j_low if r & 1 else j_low) + 2 * (1 - j_high if r & 2 else j_high)
        return pf, pj

    def remote(src, dst, ssem, rsem, r):
        pf, pj = peer(r)
        return pltpu.make_async_remote_copy(src_ref=src, dst_ref=dst, send_sem=ssem, recv_sem=rsem,
                                            device_id={'fsdp': pf, 'ep': pj}, device_id_type=MESH)

    def gate_copy(c):
        return remote(wg.at[1 - f, :, pl.ds(c * fc, fc)], gate_in.at[c], w_send.at[0, c], w_recv.at[0, c], 4)

    def up_copy(c):
        return remote(wu.at[1 - f, :, pl.ds(c * fc, fc)], up_in.at[c], w_send.at[1, c], w_recv.at[1, c], 4)

    def down_copy(q):
        return remote(wd.at[1 - f, :, pl.ds(q * dc, dc)], down_in.at[q], d_send.at[q], d_recv.at[q], 4)

    def ids_copy():
        return remote(ids, ids_oth, u_send.at[0], u_recv.at[0], 4)

    def hid_copy():
        return remote(hid, hid_oth, u_send.at[1], u_recv.at[1], 4)

    def x_copy(s, r):
        pf, pj = peer(r)
        owner = me if s == 0 else (1 - f) * 4 + j
        return remote(x_send.at[s, pj], x_all.at[pl.ds(owner * cap, cap)], x_ssem.at[s, r], x_rsem.at[s, r], r)

    def back_copy(s, chunk, r):
        pf, pj = peer(r)
        owner = (f if s == 0 else 1 - f) * 4 + pj
        return remote(o_all.at[chunk, pl.ds(owner * cap, cap)], back.at[s, chunk, pl.ds(j * cap, cap)],
                      b_send.at[s * chunks + chunk, r], b_recv.at[s * chunks + chunk, r], r)

    def y_copy(piece):
        return remote(y_own.at[piece], y_oth.at[piece], y_send.at[piece], y_recv.at[piece], 4)

    barrier = pltpu.get_barrier_semaphore()
    for r in range(1, n_dev):
        pf, pj = peer(r)
        pl.semaphore_signal(barrier, inc=1, device_id={'fsdp': pf, 'ep': pj}, device_id_type=MESH)
    pl.semaphore_wait(barrier, n_dev - 1)

    ids_copy().start()
    hid_copy().start()
    for c in range(FF_CHUNKS):
        gate_copy(c).start()
        up_copy(c).start()
    for q in range(HALF_CHUNKS):
        down_copy(q).start()

    wr_pad[...] = jnp.zeros_like(wr_pad)
    wr_pad[0:n_dev, :] = wr[...]
    tri = (lax.broadcasted_iota(jnp.int32, (TOK, TOK), 0) < lax.broadcasted_iota(jnp.int32, (TOK, TOK), 1)).astype(F32).astype(BF16)
    spot = lax.broadcasted_iota(jnp.int32, (n_dev, TOK), 0)
    column = lax.broadcasted_iota(jnp.int32, (n_dev, TOK), 1)
    line = lax.broadcasted_iota(jnp.int32, (TOK, TOK), 0)

    def route(s, ids_ref, blk, carry):
        count, bases = carry
        here = pl.ds(pl.multiple_of(blk * TOK, TOK), TOK)
        id0, id1 = ids_ref[0:1, here], ids_ref[1:2, here]
        place0 = lax.rem(id0, 2) * 4 + lax.div(id0, 2)
        place1 = lax.rem(id1, 2) * 4 + lax.div(id1, 2)
        chosen = (spot == place0) | (spot == place1)
        before = jnp.dot(jnp.where(chosen, 1.0, 0.0).astype(BF16), tri, preferred_element_type=F32)
        position = before.astype(jnp.int32) + count
        kept = jnp.where(chosen & (position < cap), position, -1)
        rows[:, here] = kept
        mine = (spot >= f * 4) & (spot < f * 4 + 4)
        flat = jnp.where(mine & (kept >= 0), kept + (spot - f * 4) * cap, -1)
        slot0 = jnp.sum(jnp.where(spot == place0, flat, 0), axis=0, keepdims=True)
        slot1 = jnp.sum(jnp.where(spot == place1, flat, 0), axis=0, keepdims=True)
        stacked = jnp.where(line == 0, id0, jnp.where(line == 1, id1, jnp.where(line == 2, slot0, slot1)))
        meta[s, here, :] = stacked.astype(F32).T.astype(jnp.int32)
        start = jnp.minimum(lax.div(count, 16), (cap - WINDOW) // 16)
        bases = jnp.where(column == blk, start + lax.rem(spot, 4) * (cap // 16), bases)
        return count + jnp.sum(jnp.where(chosen, 1, 0), axis=1, keepdims=True), bases

    def dispatch(u_buf, x_buf, onehot):
        block = 128
        gain_row = gain[...].astype(F32)[None, :]
        lane = lax.broadcasted_iota(jnp.int32, (block, 128), 1)

        for s in range(2):
            owner = me if s == 0 else (1 - f) * 4 + j
            if s == 1:
                ids_copy().wait_recv()
                hid_copy().wait_recv()
            load = pltpu.make_async_copy(hid if s == 0 else hid_oth, x_buf.at[pl.ds(0, tok)], local_sem.at[0])
            load.start()
            base_v[s] = lax.fori_loop(0, n_blocks, functools.partial(route, s, ids if s == 0 else ids_oth),
                                      (jnp.zeros((n_dev, 1), jnp.int32), jnp.zeros((n_dev, TOK), jnp.int32)))[1]
            load.wait()

            @pl.loop(0, tok // block)
            def _(i):
                here = pl.ds(pl.multiple_of(i * block, block), block)
                x = x_buf[here, :].astype(F32)
                mean_sq = jnp.mean(x * x, axis=-1, keepdims=True)
                u = (x * lax.rsqrt(mean_sq + EPS) * gain_row).astype(BF16)
                u_buf[here, :] = u
                logits = lax.dot_general(u, wr_pad[...], (((1,), (1,)), ((), ())), preferred_element_type=F32)
                info = meta[s, here, :]
                l0 = jnp.sum(jnp.where(lane == info[:, 0:1], logits, 0.0), axis=1, keepdims=True)
                l1 = jnp.sum(jnp.where(lane == info[:, 1:2], logits, 0.0), axis=1, keepdims=True)
                top = jnp.maximum(l0, l1)
                e0, e1 = jnp.exp(l0 - top), jnp.exp(l1 - top)
                total = e0 + e1
                probs[s, here, :] = jnp.where(lane == 0, e0 / total, e1 / total)

            @pl.loop(0, 4)
            def _(p):
                row = rows[pl.ds(f * 4 + p, 1), :]
                slot = lax.broadcasted_iota(jnp.int32, (cap, tok), 0)
                onehot[...] = jnp.where(slot == row, 1.0, 0.0).astype(BF16)

                @pl.loop(0, d_model // 256)
                def _(n):
                    cols = pl.ds(pl.multiple_of(n * 256, 256), 256)
                    x_buf[pl.ds(pl.multiple_of(p * cap, cap), cap), cols] = jnp.dot(
                        onehot[...], u_buf[:, cols], preferred_element_type=F32).astype(BF16)

                done = x_buf.at[pl.ds(pl.multiple_of(p * cap, cap), cap)]

                @pl.when(p == j)
                def _():
                    pltpu.make_async_copy(done, x_all.at[pl.ds(owner * cap, cap)], local_sem.at[p]).start()

                @pl.when(p != j)
                def _():
                    pltpu.make_async_copy(done, x_send.at[s, p], local_sem.at[p]).start()

            for p in range(4):
                pltpu.make_async_copy(x_buf.at[pl.ds(p * cap, cap)], x_send.at[s, p], local_sem.at[p]).wait()
            for r in (1, 2, 3):
                x_copy(s, r).start()

        move = pltpu.make_async_copy(base_v, base_s, local_sem.at[0])
        move.start()
        move.wait()

    pl.run_scoped(dispatch, pltpu.VMEM((tok, d_model), BF16), pltpu.VMEM((4 * cap, d_model), BF16), pltpu.VMEM((cap, tok), BF16))

    for s in range(2):
        for r in (1, 2, 3):
            x_copy(s, r).wait_recv()

    bm = 512
    sub = 256

    @pl.loop(0, FF_CHUNKS)
    def _(c):
        gate_copy(c).wait_recv()
        up_copy(c).wait_recv()

        def body(x_own, x_oth, g_own, g_oth, p_own, p_oth, h_ref):
            @pl.loop(0, bm // sub)
            def _(i):
                here = pl.ds(pl.multiple_of(i * sub, sub), sub)
                lhs_own, lhs_oth = x_own[here, :], x_oth[here, :]
                a = jnp.dot(lhs_own, g_own[...], preferred_element_type=F32) + jnp.dot(lhs_oth, g_oth[...], preferred_element_type=F32)
                b = jnp.dot(lhs_own, p_own[...], preferred_element_type=F32) + jnp.dot(lhs_oth, p_oth[...], preferred_element_type=F32)
                h_ref[here, :] = (a * jax.nn.sigmoid(a) * b).astype(BF16)

        pltpu.emit_pipeline(
            body, grid=(n_rows // bm,),
            in_specs=[pl.BlockSpec((bm, half), lambda i: (i, f)), pl.BlockSpec((bm, half), lambda i: (i, 1 - f)),
                      pl.BlockSpec((half, fc), lambda i: (0, c)), pl.BlockSpec((half, fc), lambda i: (0, 0)),
                      pl.BlockSpec((half, fc), lambda i: (0, c)), pl.BlockSpec((half, fc), lambda i: (0, 0))],
            out_specs=[pl.BlockSpec((bm, fc), lambda i: (i, c))],
        )(x_all, x_all, wg.at[f], gate_in.at[c], wu.at[f], up_in.at[c], h_all)

    def project(h_ref, w_ref, o_ref):
        @pl.loop(0, bm // sub)
        def _(i):
            here = pl.ds(pl.multiple_of(i * sub, sub), sub)
            o_ref[here, :] = jnp.dot(h_ref[here, :], w_ref[...], preferred_element_type=F32).astype(BF16)

    def finish(picks, segs, mix, seg_piece, mix_piece, y_piece, window, window_piece):
        side_rows = 4 * WINDOW
        lane = lax.broadcasted_iota(jnp.int32, (1, side_rows), 1)

        def expert_out(phase, q):
            if phase == 0:
                weight, col, chunk = wd.at[f], q, f * HALF_CHUNKS + q
            else:
                down_copy(q).wait_recv()
                weight, col, chunk = down_in.at[q], 0, (1 - f) * HALF_CHUNKS + q
            pltpu.emit_pipeline(
                project, grid=(n_rows // bm,),
                in_specs=[pl.BlockSpec((bm, ff), lambda i: (i, 0)), pl.BlockSpec((ff, dc), lambda i: (0, col))],
                out_specs=[pl.BlockSpec((bm, dc), lambda i: (i, 0))],
            )(h_all, weight, o_all.at[chunk])
            for s in (1, 0):
                for r in (1, 2, 3):
                    back_copy(s, chunk, r).start()

        def fill(s, chunk, cols, buf):
            moves = []
            for r in range(4):
                pj = peer(r)[1]
                owner = (f if s == 0 else 1 - f) * 4 + j
                src = back.at[s, chunk, pl.ds(pj * cap, cap), cols] if r else o_all.at[chunk, pl.ds(owner * cap, cap), cols]
                moves.append(pltpu.make_async_copy(src, buf.at[pl.ds(pj * cap, cap)], local_sem.at[2 + r]))
            return moves

        def take(s, i, buf, win):
            for p in range(4):
                win[p * WINDOW:(p + 1) * WINDOW, :] = buf[pl.ds(base_s[s, f * 4 + p, i] * 16, WINDOW), :]
            picked = jnp.dot(picks[s, i], win[...], preferred_element_type=F32)
            return picked[:TOK], picked[TOK:]

        def relay(half_id, q):
            chunk = half_id * HALF_CHUNKS + q
            for r in (1, 2, 3):
                back_copy(1, chunk, r).wait_recv()
            cols = pl.ds(pl.multiple_of(chunk * dc, PIECE), dc)
            moves = fill(1, chunk, pl.ds(0, dc), segs) + [pltpu.make_async_copy(hid_oth.at[:, cols], mix, local_sem.at[0])]
            for move in moves:
                move.start()
            for move in moves:
                move.wait()

            @pl.loop(0, n_blocks)
            def _(i):
                here = pl.ds(pl.multiple_of(i * TOK, TOK), TOK)
                r0, r1 = take(1, i, segs, window)
                info, p = meta[1, here, :], probs[1, here, :]
                both = (lax.rem(info[:, 0:1], 2) == f) & (lax.rem(info[:, 1:2], 2) == f)
                whole = mix[here, :].astype(F32) + (p[:, 0:1] * r0 + p[:, 1:2] * r1)
                mix[here, :] = jnp.where(both, whole, r0 + r1).astype(BF16)

            moves = [pltpu.make_async_copy(mix.at[:, pl.ds(k * PIECE, PIECE)], y_own.at[chunk * pieces + k], local_sem.at[k]) for k in range(pieces)]
            for move in moves:
                move.start()
            for move in moves:
                move.wait()
            for k in range(pieces):
                y_copy(chunk * pieces + k).start()

        def final(half_id, step):
            q, k = lax.div(step, pieces), lax.rem(step, pieces)
            chunk = half_id * HALF_CHUNKS + q
            piece = chunk * pieces + k
            cols = pl.ds(pl.multiple_of(piece * PIECE, PIECE), PIECE)
            moves = fill(0, chunk, pl.ds(pl.multiple_of(k * PIECE, PIECE), PIECE), seg_piece) + [pltpu.make_async_copy(hid.at[:, cols], mix_piece, local_sem.at[0])]

            @pl.when(k == 0)
            def _():
                for r in (1, 2, 3):
                    back_copy(0, chunk, r).wait_recv()

            for move in moves:
                move.start()
            y_copy(piece).wait_recv()
            load = pltpu.make_async_copy(y_oth.at[piece], y_piece, local_sem.at[1])
            load.start()
            for move in moves:
                move.wait()
            load.wait()

            @pl.loop(0, n_blocks)
            def _(i):
                here = pl.ds(pl.multiple_of(i * TOK, TOK), TOK)
                r0, r1 = take(0, i, seg_piece, window_piece)
                info, p = meta[0, here, :], probs[0, here, :]
                near0, near1 = lax.rem(info[:, 0:1], 2) == f, lax.rem(info[:, 1:2], 2) == f
                far = y_piece[here, :].astype(F32)
                c0, c1 = jnp.where(near0, r0, far), jnp.where(near1, r1, far)
                whole = mix_piece[here, :].astype(F32) + (p[:, 0:1] * c0 + p[:, 1:2] * c1)
                mix_piece[here, :] = jnp.where(near0 | near1, whole, far).astype(BF16)

            store = pltpu.make_async_copy(mix_piece, out.at[:, cols], local_sem.at[0])
            store.start()
            store.wait()

        for s in range(2):
            @pl.loop(0, n_blocks)
            def _(i):
                shift = jnp.zeros_like(lane)
                for p in range(4):
                    shift = jnp.where(lane >= p * WINDOW, base_s[s, f * 4 + p, i] * 16 - p * WINDOW, shift)
                row = lane + shift
                info = meta[s, pl.ds(pl.multiple_of(i * TOK, TOK), TOK), :]
                for k in range(2):
                    picks[s, i, k * TOK:(k + 1) * TOK, :] = jnp.where(row == info[:, 2 + k:3 + k], 1.0, 0.0).astype(BF16)

        @pl.loop(0, HALF_CHUNKS)
        def _(q):
            expert_out(0, q)

        @pl.loop(0, HALF_CHUNKS)
        def _(q):
            expert_out(1, q)

            @pl.when(q == 0)
            def _():
                @pl.loop(0, HALF_CHUNKS)
                def _(z):
                    relay(f, z)

        @pl.loop(0, HALF_CHUNKS)
        def _(q):
            relay(1 - f, q)

        @pl.loop(0, 2 * HALF_CHUNKS * pieces)
        def _(step):
            late = lax.div(step, HALF_CHUNKS * pieces)
            final(jnp.where(late == 0, 1 - f, f), lax.rem(step, HALF_CHUNKS * pieces))

    pl.run_scoped(finish, pltpu.VMEM((2, n_blocks, 2 * TOK, 4 * WINDOW), BF16), pltpu.VMEM((4 * cap, dc), BF16), pltpu.VMEM((tok, dc), BF16),
                  pltpu.VMEM((4 * cap, PIECE), BF16), pltpu.VMEM((tok, PIECE), BF16), pltpu.VMEM((tok, PIECE), BF16),
                  pltpu.VMEM((4 * WINDOW, dc), BF16), pltpu.VMEM((4 * WINDOW, PIECE), BF16))

    ids_copy().wait_send()
    hid_copy().wait_send()
    for c in range(FF_CHUNKS):
        gate_copy(c).wait_send()
        up_copy(c).wait_send()
    for q in range(HALF_CHUNKS):
        down_copy(q).wait_send()
    for s in range(2):
        for r in (1, 2, 3):
            x_copy(s, r).wait_send()

    @pl.loop(0, chunks)
    def _(chunk):
        for s in range(2):
            for r in (1, 2, 3):
                back_copy(s, chunk, r).wait_send()
        for k in range(pieces):
            y_copy(chunk * pieces + k).wait_send()


def local_block(hidden, norm_gain, w_router, w_gate, w_up, w_down, top2_ids):
    tok, d_model = hidden.shape
    num_experts = w_router.shape[1]
    half, ff = w_gate.shape[1:]
    cap = (5 * tok + 2 * num_experts - 1) // (2 * num_experts)
    fc, dc = ff // FF_CHUNKS, half // HALF_CHUNKS
    n_rows = num_experts * cap
    shape = lambda *s: jax.ShapeDtypeStruct(s, BF16)
    dma = pltpu.SemaphoreType.DMA
    results = pl.pallas_call(
        functools.partial(moe_kernel, cap),
        out_shape=[shape(tok, d_model), shape(tok, d_model),
                   shape(FF_CHUNKS, half, fc), shape(FF_CHUNKS, half, fc), shape(HALF_CHUNKS, ff, dc),
                   shape(2, 4, cap, d_model), shape(n_rows, d_model), shape(n_rows, ff),
                   shape(2 * HALF_CHUNKS, n_rows, dc), shape(2, 2 * HALF_CHUNKS, 4 * cap, dc),
                   shape(d_model // PIECE, tok, PIECE), shape(d_model // PIECE, tok, PIECE)],
        in_specs=[ANY, VMEM, VMEM, VMEM, ANY, ANY, ANY],
        out_specs=[ANY] * 12,
        scratch_shapes=[
            pltpu.VMEM((num_experts, tok), jnp.int32), pltpu.VMEM((2, tok), jnp.int32),
            pltpu.VMEM((2, tok, 128), jnp.int32), pltpu.VMEM((2, tok, 128), F32), pltpu.VMEM((128, d_model), BF16),
            pltpu.VMEM((2, num_experts, TOK), jnp.int32), pltpu.SMEM((2, num_experts, TOK), jnp.int32),
            dma((6,)), dma((2, FF_CHUNKS)), dma((2, FF_CHUNKS)), dma((HALF_CHUNKS,)), dma((HALF_CHUNKS,)),
            dma((2,)), dma((2,)), dma((2, 4)), dma((2, 4)),
            dma((4 * HALF_CHUNKS, 4)), dma((4 * HALF_CHUNKS, 4)), dma((d_model // PIECE,)), dma((d_model // PIECE,))],
        compiler_params=pltpu.CompilerParams(collective_id=0, has_side_effects=True, vmem_limit_bytes=62 * 1024 * 1024),
    )(hidden, norm_gain, w_router.T, top2_ids.T, w_gate, w_up, w_down)
    return results[0]


def solution(mesh):
    tok_spec = P(('dp', 'fsdp', 'ep'), None)
    in_specs = (tok_spec, P(None), P(None, None), P('ep', 'fsdp', None), P('ep', 'fsdp', None), P('ep', None, 'fsdp'), tok_spec)
    return jax.shard_map(local_block, mesh=mesh, in_specs=in_specs, out_specs=tok_spec, check_vma=False)
```

```python
import functools

import jax
import jax.numpy as jnp
from jax import lax
from jax.experimental import pallas as pl
from jax.experimental.pallas import tpu as pltpu
from jax.sharding import PartitionSpec as P

EPS = 1e-5
MESH = pl.DeviceIdType.MESH
ANY = pl.BlockSpec(memory_space=pl.ANY)
VMEM = pl.BlockSpec(memory_space=pltpu.VMEM)
F32 = jnp.float32
BF16 = jnp.bfloat16
FF_CHUNKS = 5
HALF_CHUNKS = 3
PIECE = 128
TOK = 128
WINDOW = TOK + 16


def moe_kernel(cap, hid, gain, wr, ids, wg, wu, wd,
               out, y_oth, near, rule, hid_oth, gate_in, up_in, down_in, x_send, x_all, h_all, o_all, back, y_own,
               rows, ids_oth, meta, probs, wr_pad, base_v, base_s, local_sem, w_send, w_recv, d_send, d_recv,
               u_send, u_recv, x_ssem, x_rsem, b_send, b_recv, y_send, y_recv):
    tok, d_model = hid.shape
    half = d_model // 2
    ff = wg.shape[2]
    fc = ff // FF_CHUNKS
    dc = half // HALF_CHUNKS
    n_dev = 8
    pieces = dc // PIECE
    n_rows = n_dev * cap
    chunks = 2 * HALF_CHUNKS
    n_blocks = tok // TOK
    f = lax.axis_index('fsdp')
    j = lax.axis_index('ep')
    me = f * 4 + j
    j_low, j_high = lax.rem(j, 2), lax.div(j, 2)

    def peer(r):
        pf = 1 - f if r // 4 else f
        pj = (1 - j_low if r & 1 else j_low) + 2 * (1 - j_high if r & 2 else j_high)
        return pf, pj

    def remote(src, dst, ssem, rsem, r):
        pf, pj = peer(r)
        return pltpu.make_async_remote_copy(src_ref=src, dst_ref=dst, send_sem=ssem, recv_sem=rsem,
                                            device_id={'fsdp': pf, 'ep': pj}, device_id_type=MESH)

    def gate_copy(c):
        return remote(wg.at[1 - f, :, pl.ds(c * fc, fc)], gate_in.at[c], w_send.at[0, c], w_recv.at[0, c], 4)

    def up_copy(c):
        return remote(wu.at[1 - f, :, pl.ds(c * fc, fc)], up_in.at[c], w_send.at[1, c], w_recv.at[1, c], 4)

    def down_copy(q):
        return remote(wd.at[1 - f, :, pl.ds(q * dc, dc)], down_in.at[q], d_send.at[q], d_recv.at[q], 4)

    def ids_copy():
        return remote(ids, ids_oth, u_send.at[0], u_recv.at[0], 4)

    def hid_copy():
        return remote(hid, hid_oth, u_send.at[1], u_recv.at[1], 4)

    def x_copy(s, r):
        pf, pj = peer(r)
        owner = me if s == 0 else (1 - f) * 4 + j
        return remote(x_send.at[s, pj], x_all.at[pl.ds(owner * cap, cap)], x_ssem.at[s, r], x_rsem.at[s, r], r)

    def back_copy(s, chunk, r):
        pf, pj = peer(r)
        owner = (f if s == 0 else 1 - f) * 4 + pj
        return remote(o_all.at[chunk, pl.ds(owner * cap, cap)], back.at[s, chunk, pl.ds(j * cap, cap)],
                      b_send.at[s * chunks + chunk, r], b_recv.at[s * chunks + chunk, r], r)

    def y_copy(piece):
        return remote(y_own.at[piece], y_oth.at[piece], y_send.at[piece], y_recv.at[piece], 4)

    barrier = pltpu.get_barrier_semaphore()
    for r in range(1, n_dev):
        pf, pj = peer(r)
        pl.semaphore_signal(barrier, inc=1, device_id={'fsdp': pf, 'ep': pj}, device_id_type=MESH)
    pl.semaphore_wait(barrier, n_dev - 1)

    ids_copy().start()
    hid_copy().start()
    for c in range(FF_CHUNKS):
        gate_copy(c).start()
        up_copy(c).start()
    for q in range(HALF_CHUNKS):
        down_copy(q).start()

    wr_pad[...] = jnp.zeros_like(wr_pad)
    wr_pad[0:n_dev, :] = wr[...]
    tri = (lax.broadcasted_iota(jnp.int32, (TOK, TOK), 0) < lax.broadcasted_iota(jnp.int32, (TOK, TOK), 1)).astype(F32).astype(BF16)
    spot = lax.broadcasted_iota(jnp.int32, (n_dev, TOK), 0)
    column = lax.broadcasted_iota(jnp.int32, (n_dev, TOK), 1)
    line = lax.broadcasted_iota(jnp.int32, (TOK, TOK), 0)

    def route(s, ids_ref, blk, carry):
        count, bases = carry
        here = pl.ds(pl.multiple_of(blk * TOK, TOK), TOK)
        id0, id1 = ids_ref[0:1, here], ids_ref[1:2, here]
        place0 = lax.rem(id0, 2) * 4 + lax.div(id0, 2)
        place1 = lax.rem(id1, 2) * 4 + lax.div(id1, 2)
        chosen = (spot == place0) | (spot == place1)
        before = jnp.dot(jnp.where(chosen, 1.0, 0.0).astype(BF16), tri, preferred_element_type=F32)
        position = before.astype(jnp.int32) + count
        kept = jnp.where(chosen & (position < cap), position, -1)
        rows[:, here] = kept
        mine = (spot >= f * 4) & (spot < f * 4 + 4)
        flat = jnp.where(mine & (kept >= 0), kept + (spot - f * 4) * cap, -1)
        slot0 = jnp.sum(jnp.where(spot == place0, flat, 0), axis=0, keepdims=True)
        slot1 = jnp.sum(jnp.where(spot == place1, flat, 0), axis=0, keepdims=True)
        stacked = jnp.where(line == 0, id0, jnp.where(line == 1, id1, jnp.where(line == 2, slot0, slot1)))
        meta[s, here, :] = stacked.astype(F32).T.astype(jnp.int32)
        start = jnp.minimum(lax.div(count, 16), (cap - WINDOW) // 16)
        bases = jnp.where(column == blk, start + lax.rem(spot, 4) * (cap // 16), bases)
        return count + jnp.sum(jnp.where(chosen, 1, 0), axis=1, keepdims=True), bases

    def dispatch(u_buf, x_buf, onehot):
        block = 128
        gain_row = gain[...].astype(F32)[None, :]
        lane = lax.broadcasted_iota(jnp.int32, (block, 128), 1)

        for s in range(2):
            owner = me if s == 0 else (1 - f) * 4 + j
            if s == 1:
                ids_copy().wait_recv()
                hid_copy().wait_recv()
            load = pltpu.make_async_copy(hid if s == 0 else hid_oth, x_buf.at[pl.ds(0, tok)], local_sem.at[0])
            load.start()
            base_v[s] = lax.fori_loop(0, n_blocks, functools.partial(route, s, ids if s == 0 else ids_oth),
                                      (jnp.zeros((n_dev, 1), jnp.int32), jnp.zeros((n_dev, TOK), jnp.int32)))[1]
            load.wait()

            @pl.loop(0, tok // block)
            def _(i):
                here = pl.ds(pl.multiple_of(i * block, block), block)
                x = x_buf[here, :].astype(F32)
                mean_sq = jnp.mean(x * x, axis=-1, keepdims=True)
                u = (x * lax.rsqrt(mean_sq + EPS) * gain_row).astype(BF16)
                u_buf[here, :] = u
                logits = lax.dot_general(u, wr_pad[...], (((1,), (1,)), ((), ())), preferred_element_type=F32)
                info = meta[s, here, :]
                l0 = jnp.sum(jnp.where(lane == info[:, 0:1], logits, 0.0), axis=1, keepdims=True)
                l1 = jnp.sum(jnp.where(lane == info[:, 1:2], logits, 0.0), axis=1, keepdims=True)
                top = jnp.maximum(l0, l1)
                e0, e1 = jnp.exp(l0 - top), jnp.exp(l1 - top)
                total = e0 + e1
                probs[s, here, :] = jnp.where(lane == 0, e0 / total, e1 / total)

            @pl.loop(0, 4)
            def _(p):
                row = rows[pl.ds(f * 4 + p, 1), :]
                slot = lax.broadcasted_iota(jnp.int32, (cap, tok), 0)
                onehot[...] = jnp.where(slot == row, 1.0, 0.0).astype(BF16)

                @pl.loop(0, d_model // 256)
                def _(n):
                    cols = pl.ds(pl.multiple_of(n * 256, 256), 256)
                    x_buf[pl.ds(pl.multiple_of(p * cap, cap), cap), cols] = jnp.dot(
                        onehot[...], u_buf[:, cols], preferred_element_type=F32).astype(BF16)

                done = x_buf.at[pl.ds(pl.multiple_of(p * cap, cap), cap)]

                @pl.when(p == j)
                def _():
                    pltpu.make_async_copy(done, x_all.at[pl.ds(owner * cap, cap)], local_sem.at[p]).start()

                @pl.when(p != j)
                def _():
                    pltpu.make_async_copy(done, x_send.at[s, p], local_sem.at[p]).start()

            for p in range(4):
                pltpu.make_async_copy(x_buf.at[pl.ds(p * cap, cap)], x_send.at[s, p], local_sem.at[p]).wait()
            for r in (1, 2, 3):
                x_copy(s, r).start()

        move = pltpu.make_async_copy(base_v, base_s, local_sem.at[0])
        move.start()
        move.wait()

    pl.run_scoped(dispatch, pltpu.VMEM((tok, d_model), BF16), pltpu.VMEM((4 * cap, d_model), BF16), pltpu.VMEM((cap, tok), BF16))

    for s in range(2):
        for r in (1, 2, 3):
            x_copy(s, r).wait_recv()

    bm = 512
    sub = 256

    @pl.loop(0, FF_CHUNKS)
    def _(c):
        gate_copy(c).wait_recv()
        up_copy(c).wait_recv()

        def body(x_own, x_oth, g_own, g_oth, p_own, p_oth, h_ref):
            @pl.loop(0, bm // sub)
            def _(i):
                here = pl.ds(pl.multiple_of(i * sub, sub), sub)
                lhs_own, lhs_oth = x_own[here, :], x_oth[here, :]
                a = jnp.dot(lhs_own, g_own[...], preferred_element_type=F32) + jnp.dot(lhs_oth, g_oth[...], preferred_element_type=F32)
                b = jnp.dot(lhs_own, p_own[...], preferred_element_type=F32) + jnp.dot(lhs_oth, p_oth[...], preferred_element_type=F32)
                h_ref[here, :] = (a * jax.nn.sigmoid(a) * b).astype(BF16)

        pltpu.emit_pipeline(
            body, grid=(n_rows // bm,),
            in_specs=[pl.BlockSpec((bm, half), lambda i: (i, f)), pl.BlockSpec((bm, half), lambda i: (i, 1 - f)),
                      pl.BlockSpec((half, fc), lambda i: (0, c)), pl.BlockSpec((half, fc), lambda i: (0, 0)),
                      pl.BlockSpec((half, fc), lambda i: (0, c)), pl.BlockSpec((half, fc), lambda i: (0, 0))],
            out_specs=[pl.BlockSpec((bm, fc), lambda i: (i, c))],
        )(x_all, x_all, wg.at[f], gate_in.at[c], wu.at[f], up_in.at[c], h_all)

    def project(h_ref, w_ref, o_ref):
        @pl.loop(0, bm // sub)
        def _(i):
            here = pl.ds(pl.multiple_of(i * sub, sub), sub)
            o_ref[here, :] = jnp.dot(h_ref[here, :], w_ref[...], preferred_element_type=F32).astype(BF16)

    def finish(picks, segs, mix, seg_piece, mix_piece, y_piece, window, window_piece):
        side_rows = 4 * WINDOW
        lane = lax.broadcasted_iota(jnp.int32, (1, side_rows), 1)

        def expert_out(phase, q):
            if phase == 0:
                weight, col, chunk = wd.at[f], q, f * HALF_CHUNKS + q
            else:
                down_copy(q).wait_recv()
                weight, col, chunk = down_in.at[q], 0, (1 - f) * HALF_CHUNKS + q
            pltpu.emit_pipeline(
                project, grid=(n_rows // bm,),
                in_specs=[pl.BlockSpec((bm, ff), lambda i: (i, 0)), pl.BlockSpec((ff, dc), lambda i: (0, col))],
                out_specs=[pl.BlockSpec((bm, dc), lambda i: (i, 0))],
            )(h_all, weight, o_all.at[chunk])
            for s in (1, 0):
                for r in (1, 2, 3):
                    back_copy(s, chunk, r).start()

        def fill(s, chunk, cols, buf):
            moves = []
            for r in range(4):
                pj = peer(r)[1]
                owner = (f if s == 0 else 1 - f) * 4 + j
                src = back.at[s, chunk, pl.ds(pj * cap, cap), cols] if r else o_all.at[chunk, pl.ds(owner * cap, cap), cols]
                moves.append(pltpu.make_async_copy(src, buf.at[pl.ds(pj * cap, cap)], local_sem.at[2 + r]))
            return moves

        def take(s, i, buf, win):
            for p in range(4):
                win[p * WINDOW:(p + 1) * WINDOW, :] = buf[pl.ds(base_s[s, f * 4 + p, i] * 16, WINDOW), :]
            picked = jnp.dot(picks[s, i], win[...], preferred_element_type=F32)
            return picked[:TOK], picked[TOK:]

        def relay(half_id, q):
            chunk = half_id * HALF_CHUNKS + q
            for r in (1, 2, 3):
                back_copy(1, chunk, r).wait_recv()
            cols = pl.ds(pl.multiple_of(chunk * dc, PIECE), dc)
            moves = fill(1, chunk, pl.ds(0, dc), segs) + [pltpu.make_async_copy(hid_oth.at[:, cols], mix, local_sem.at[0])]
            for move in moves:
                move.start()
            for move in moves:
                move.wait()

            @pl.loop(0, n_blocks)
            def _(i):
                here = pl.ds(pl.multiple_of(i * TOK, TOK), TOK)
                r0, r1 = take(1, i, segs, window)
                info, p = meta[1, here, :], probs[1, here, :]
                both = (lax.rem(info[:, 0:1], 2) == f) & (lax.rem(info[:, 1:2], 2) == f)
                whole = mix[here, :].astype(F32) + (p[:, 0:1] * r0 + p[:, 1:2] * r1)
                mix[here, :] = jnp.where(both, whole, r0 + r1).astype(BF16)

            moves = [pltpu.make_async_copy(mix.at[:, pl.ds(k * PIECE, PIECE)], y_own.at[chunk * pieces + k], local_sem.at[k]) for k in range(pieces)]
            for move in moves:
                move.start()
            for move in moves:
                move.wait()
            for k in range(pieces):
                y_copy(chunk * pieces + k).start()

        def near_rows(half_id, q, k):
            chunk = half_id * HALF_CHUNKS + q

            @pl.when(k == 0)
            def _():
                for r in (1, 2, 3):
                    back_copy(0, chunk, r).wait_recv()

            return fill(0, chunk, pl.ds(pl.multiple_of(k * PIECE, PIECE), PIECE), seg_piece)

        def near_far(i):
            here = pl.ds(pl.multiple_of(i * TOK, TOK), TOK)
            r0, r1 = take(0, i, seg_piece, window_piece)
            info, p = meta[0, here, :], probs[0, here, :]
            near0, near1 = lax.rem(info[:, 0:1], 2) == f, lax.rem(info[:, 1:2], 2) == f
            return here, r0, r1, near0, near1, p[:, 0:1], p[:, 1:2]

        def final(half_id, step):
            q, k = lax.div(step, pieces), lax.rem(step, pieces)
            piece = (half_id * HALF_CHUNKS + q) * pieces + k
            cols = pl.ds(pl.multiple_of(piece * PIECE, PIECE), PIECE)
            moves = near_rows(half_id, q, k) + [pltpu.make_async_copy(hid.at[:, cols], mix_piece, local_sem.at[0])]
            for move in moves:
                move.start()
            y_copy(piece).wait_recv()
            load = pltpu.make_async_copy(y_oth.at[piece], y_piece, local_sem.at[1])
            load.start()
            for move in moves:
                move.wait()
            load.wait()

            @pl.loop(0, n_blocks)
            def _(i):
                here, r0, r1, near0, near1, p0, p1 = near_far(i)
                far = y_piece[here, :].astype(F32)
                c0, c1 = jnp.where(near0, r0, far), jnp.where(near1, r1, far)
                whole = mix_piece[here, :].astype(F32) + (p0 * c0 + p1 * c1)
                mix_piece[here, :] = jnp.where(near0 | near1, whole, far).astype(BF16)

            store = pltpu.make_async_copy(mix_piece, out.at[:, cols], local_sem.at[0])
            store.start()
            store.wait()

        def leave_last(near_buf, rule_buf):
            last = HALF_CHUNKS * pieces - 1
            moves = near_rows(f, last // pieces, last % pieces)
            for move in moves:
                move.start()
            for move in moves:
                move.wait()
            lanes = lax.broadcasted_iota(jnp.int32, (TOK, PIECE), 1)

            @pl.loop(0, n_blocks)
            def _(i):
                here, r0, r1, near0, near1, p0, p1 = near_far(i)
                near_buf[here, :] = p0 * jnp.where(near0, r0, 0.0) + p1 * jnp.where(near1, r1, 0.0)
                p_far = jnp.where(near0, jnp.where(near1, 0.0, p1), p0)
                all_far = jnp.where(near0 | near1, 0.0, 1.0)
                rule_buf[here, :] = jnp.where(lanes == 0, p_far, all_far)

            moves = [pltpu.make_async_copy(near_buf, near, local_sem.at[0]), pltpu.make_async_copy(rule_buf, rule, local_sem.at[1])]
            for move in moves:
                move.start()
            for move in moves:
                move.wait()
            y_copy(f * HALF_CHUNKS * pieces + last).wait_recv()

        for s in range(2):
            @pl.loop(0, n_blocks)
            def _(i):
                shift = jnp.zeros_like(lane)
                for p in range(4):
                    shift = jnp.where(lane >= p * WINDOW, base_s[s, f * 4 + p, i] * 16 - p * WINDOW, shift)
                row = lane + shift
                info = meta[s, pl.ds(pl.multiple_of(i * TOK, TOK), TOK), :]
                for k in range(2):
                    picks[s, i, k * TOK:(k + 1) * TOK, :] = jnp.where(row == info[:, 2 + k:3 + k], 1.0, 0.0).astype(BF16)

        @pl.loop(0, HALF_CHUNKS)
        def _(q):
            expert_out(0, q)

        @pl.loop(0, HALF_CHUNKS)
        def _(q):
            expert_out(1, q)

            @pl.when(q == 0)
            def _():
                @pl.loop(0, HALF_CHUNKS)
                def _(z):
                    relay(f, z)

        @pl.loop(0, HALF_CHUNKS)
        def _(q):
            relay(1 - f, q)

        @pl.loop(0, 2 * HALF_CHUNKS * pieces - 1)
        def _(step):
            late = lax.div(step, HALF_CHUNKS * pieces)
            final(jnp.where(late == 0, 1 - f, f), lax.rem(step, HALF_CHUNKS * pieces))

        pl.run_scoped(leave_last, pltpu.VMEM((tok, PIECE), F32), pltpu.VMEM((tok, PIECE), F32))

    pl.run_scoped(finish, pltpu.VMEM((2, n_blocks, 2 * TOK, 4 * WINDOW), BF16), pltpu.VMEM((4 * cap, dc), BF16), pltpu.VMEM((tok, dc), BF16),
                  pltpu.VMEM((4 * cap, PIECE), BF16), pltpu.VMEM((tok, PIECE), BF16), pltpu.VMEM((tok, PIECE), BF16),
                  pltpu.VMEM((4 * WINDOW, dc), BF16), pltpu.VMEM((4 * WINDOW, PIECE), BF16))

    ids_copy().wait_send()
    hid_copy().wait_send()
    for c in range(FF_CHUNKS):
        gate_copy(c).wait_send()
        up_copy(c).wait_send()
    for q in range(HALF_CHUNKS):
        down_copy(q).wait_send()
    for s in range(2):
        for r in (1, 2, 3):
            x_copy(s, r).wait_send()

    @pl.loop(0, chunks)
    def _(chunk):
        for s in range(2):
            for r in (1, 2, 3):
                back_copy(s, chunk, r).wait_send()
        for k in range(pieces):
            y_copy(chunk * pieces + k).wait_send()


def last_piece_kernel(part, y_oth, near, rule, hid, out):
    tok, d_model = part.shape
    half = d_model // 2
    piece = (lax.axis_index('fsdp') + 1) * (half // PIECE) - 1
    cols = pl.ds(pl.multiple_of(piece * PIECE, PIECE), PIECE)

    def body(part_ref, y_ref, near_ref, rule_ref, hid_ref, out_ref):
        out_ref[...] = part_ref[...]
        far = y_ref[...].astype(F32)
        p_far, all_far = rule_ref[:, 0:1], rule_ref[:, 1:2]
        whole = hid_ref[...].astype(F32) + (near_ref[...] + p_far * far)
        out_ref[:, cols] = jnp.where(all_far > 0.0, far, whole).astype(BF16)

    block = 128
    narrow = pl.BlockSpec((block, PIECE), lambda i: (i, 0))
    wide = pl.BlockSpec((block, d_model), lambda i: (i, 0))
    pltpu.emit_pipeline(
        body, grid=(tok // block,),
        in_specs=[wide, narrow, narrow, narrow, pl.BlockSpec((block, PIECE), lambda i: (i, piece))],
        out_specs=[wide],
    )(part, y_oth.at[piece], near, rule, hid, out)


def local_block(hidden, norm_gain, w_router, w_gate, w_up, w_down, top2_ids):
    tok, d_model = hidden.shape
    num_experts = w_router.shape[1]
    half, ff = w_gate.shape[1:]
    cap = (5 * tok + 2 * num_experts - 1) // (2 * num_experts)
    fc, dc = ff // FF_CHUNKS, half // HALF_CHUNKS
    n_rows = num_experts * cap
    shape = lambda *s: jax.ShapeDtypeStruct(s, BF16)
    dma = pltpu.SemaphoreType.DMA
    results = pl.pallas_call(
        functools.partial(moe_kernel, cap),
        out_shape=[shape(tok, d_model), shape(d_model // PIECE, tok, PIECE),
                   jax.ShapeDtypeStruct((tok, PIECE), F32), jax.ShapeDtypeStruct((tok, PIECE), F32), shape(tok, d_model),
                   shape(FF_CHUNKS, half, fc), shape(FF_CHUNKS, half, fc), shape(HALF_CHUNKS, ff, dc),
                   shape(2, 4, cap, d_model), shape(n_rows, d_model), shape(n_rows, ff),
                   shape(2 * HALF_CHUNKS, n_rows, dc), shape(2, 2 * HALF_CHUNKS, 4 * cap, dc),
                   shape(d_model // PIECE, tok, PIECE)],
        in_specs=[ANY, VMEM, VMEM, VMEM, ANY, ANY, ANY],
        out_specs=[ANY] * 14,
        scratch_shapes=[
            pltpu.VMEM((num_experts, tok), jnp.int32), pltpu.VMEM((2, tok), jnp.int32),
            pltpu.VMEM((2, tok, 128), jnp.int32), pltpu.VMEM((2, tok, 128), F32), pltpu.VMEM((128, d_model), BF16),
            pltpu.VMEM((2, num_experts, TOK), jnp.int32), pltpu.SMEM((2, num_experts, TOK), jnp.int32),
            dma((6,)), dma((2, FF_CHUNKS)), dma((2, FF_CHUNKS)), dma((HALF_CHUNKS,)), dma((HALF_CHUNKS,)),
            dma((2,)), dma((2,)), dma((2, 4)), dma((2, 4)),
            dma((4 * HALF_CHUNKS, 4)), dma((4 * HALF_CHUNKS, 4)), dma((d_model // PIECE,)), dma((d_model // PIECE,))],
        compiler_params=pltpu.CompilerParams(collective_id=0, has_side_effects=True, vmem_limit_bytes=62 * 1024 * 1024),
    )(hidden, norm_gain, w_router.T, top2_ids.T, w_gate, w_up, w_down)
    return pl.pallas_call(
        last_piece_kernel, out_shape=shape(tok, d_model), in_specs=[ANY] * 5, out_specs=ANY,
        compiler_params=pltpu.CompilerParams(vmem_limit_bytes=62 * 1024 * 1024),
    )(*results[:4], hidden)


def solution(mesh):
    tok_spec = P(('dp', 'fsdp', 'ep'), None)
    in_specs = (tok_spec, P(None), P(None, None), P('ep', 'fsdp', None), P('ep', 'fsdp', None), P('ep', None, 'fsdp'), tok_spec)
    return jax.shard_map(local_block, mesh=mesh, in_specs=in_specs, out_specs=tok_spec, check_vma=False)
```

```python
import functools

import jax
import jax.numpy as jnp
from jax import lax
from jax.experimental import pallas as pl
from jax.experimental.pallas import tpu as pltpu
from jax.sharding import PartitionSpec as P

EPS = 1e-5
MESH = pl.DeviceIdType.MESH
ANY = pl.BlockSpec(memory_space=pl.ANY)
VMEM = pl.BlockSpec(memory_space=pltpu.VMEM)
F32 = jnp.float32
BF16 = jnp.bfloat16
FF_CHUNKS = 5
HALF_CHUNKS = 3
PIECE = 128
TOK = 128
WINDOW = TOK + 16


def moe_kernel(cap, hid, gain, wr, ids, wg, wu, wd,
               out, hid_oth, gate_in, up_in, down_in, x_send, x_all, h_all, o_all, back, y_own, y_oth,
               rows, ids_oth, meta, probs, wr_pad, base_v, base_s, local_sem, w_send, w_recv, d_send, d_recv,
               u_send, u_recv, x_ssem, x_rsem, b_send, b_recv, y_send, y_recv, y_sem):
    tok, d_model = hid.shape
    half = d_model // 2
    ff = wg.shape[2]
    fc = ff // FF_CHUNKS
    dc = half // HALF_CHUNKS
    n_dev = 8
    pieces = dc // PIECE
    n_rows = n_dev * cap
    chunks = 2 * HALF_CHUNKS
    n_blocks = tok // TOK
    f = lax.axis_index('fsdp')
    j = lax.axis_index('ep')
    me = f * 4 + j
    j_low, j_high = lax.rem(j, 2), lax.div(j, 2)

    def peer(r):
        pf = 1 - f if r // 4 else f
        pj = (1 - j_low if r & 1 else j_low) + 2 * (1 - j_high if r & 2 else j_high)
        return pf, pj

    def remote(src, dst, ssem, rsem, r):
        pf, pj = peer(r)
        return pltpu.make_async_remote_copy(src_ref=src, dst_ref=dst, send_sem=ssem, recv_sem=rsem,
                                            device_id={'fsdp': pf, 'ep': pj}, device_id_type=MESH)

    def gate_copy(c):
        return remote(wg.at[1 - f, :, pl.ds(c * fc, fc)], gate_in.at[c], w_send.at[0, c], w_recv.at[0, c], 4)

    def up_copy(c):
        return remote(wu.at[1 - f, :, pl.ds(c * fc, fc)], up_in.at[c], w_send.at[1, c], w_recv.at[1, c], 4)

    def down_copy(q):
        return remote(wd.at[1 - f, :, pl.ds(q * dc, dc)], down_in.at[q], d_send.at[q], d_recv.at[q], 4)

    def ids_copy():
        return remote(ids, ids_oth, u_send.at[0], u_recv.at[0], 4)

    def hid_copy():
        return remote(hid, hid_oth, u_send.at[1], u_recv.at[1], 4)

    def x_copy(s, r):
        pf, pj = peer(r)
        owner = me if s == 0 else (1 - f) * 4 + j
        return remote(x_send.at[s, pj], x_all.at[pl.ds(owner * cap, cap)], x_ssem.at[s, r], x_rsem.at[s, r], r)

    def back_copy(s, chunk, r):
        pf, pj = peer(r)
        owner = (f if s == 0 else 1 - f) * 4 + pj
        return remote(o_all.at[chunk, pl.ds(owner * cap, cap)], back.at[s, chunk, pl.ds(j * cap, cap)],
                      b_send.at[s * chunks + chunk, r], b_recv.at[s * chunks + chunk, r], r)

    def y_copy(piece):
        return remote(y_own.at[piece], y_oth.at[piece], y_send.at[piece], y_recv.at[piece], 4)

    barrier = pltpu.get_barrier_semaphore()
    for r in range(1, n_dev):
        pf, pj = peer(r)
        pl.semaphore_signal(barrier, inc=1, device_id={'fsdp': pf, 'ep': pj}, device_id_type=MESH)
    pl.semaphore_wait(barrier, n_dev - 1)

    ids_copy().start()
    hid_copy().start()
    for c in range(FF_CHUNKS):
        gate_copy(c).start()
        up_copy(c).start()
    for q in range(HALF_CHUNKS):
        down_copy(q).start()

    wr_pad[...] = jnp.zeros_like(wr_pad)
    wr_pad[0:n_dev, :] = wr[...]
    tri = (lax.broadcasted_iota(jnp.int32, (TOK, TOK), 0) < lax.broadcasted_iota(jnp.int32, (TOK, TOK), 1)).astype(F32).astype(BF16)
    spot = lax.broadcasted_iota(jnp.int32, (n_dev, TOK), 0)
    column = lax.broadcasted_iota(jnp.int32, (n_dev, TOK), 1)
    line = lax.broadcasted_iota(jnp.int32, (TOK, TOK), 0)

    def route(s, ids_ref, blk, carry):
        count, bases = carry
        here = pl.ds(pl.multiple_of(blk * TOK, TOK), TOK)
        id0, id1 = ids_ref[0:1, here], ids_ref[1:2, here]
        place0 = lax.rem(id0, 2) * 4 + lax.div(id0, 2)
        place1 = lax.rem(id1, 2) * 4 + lax.div(id1, 2)
        chosen = (spot == place0) | (spot == place1)
        before = jnp.dot(jnp.where(chosen, 1.0, 0.0).astype(BF16), tri, preferred_element_type=F32)
        position = before.astype(jnp.int32) + count
        kept = jnp.where(chosen & (position < cap), position, -1)
        rows[:, here] = kept
        mine = (spot >= f * 4) & (spot < f * 4 + 4)
        flat = jnp.where(mine & (kept >= 0), kept + (spot - f * 4) * cap, -1)
        slot0 = jnp.sum(jnp.where(spot == place0, flat, 0), axis=0, keepdims=True)
        slot1 = jnp.sum(jnp.where(spot == place1, flat, 0), axis=0, keepdims=True)
        stacked = jnp.where(line == 0, id0, jnp.where(line == 1, id1, jnp.where(line == 2, slot0, slot1)))
        meta[s, here, :] = stacked.astype(F32).T.astype(jnp.int32)
        start = jnp.minimum(lax.div(count, 16), (cap - WINDOW) // 16)
        bases = jnp.where(column == blk, start + lax.rem(spot, 4) * (cap // 16), bases)
        return count + jnp.sum(jnp.where(chosen, 1, 0), axis=1, keepdims=True), bases

    def dispatch(u_buf, x_buf, onehot):
        block = 128
        gain_row = gain[...].astype(F32)[None, :]
        lane = lax.broadcasted_iota(jnp.int32, (block, 128), 1)

        for s in range(2):
            owner = me if s == 0 else (1 - f) * 4 + j
            if s == 1:
                ids_copy().wait_recv()
                hid_copy().wait_recv()
            load = pltpu.make_async_copy(hid if s == 0 else hid_oth, x_buf.at[pl.ds(0, tok)], local_sem.at[0])
            load.start()
            base_v[s] = lax.fori_loop(0, n_blocks, functools.partial(route, s, ids if s == 0 else ids_oth),
                                      (jnp.zeros((n_dev, 1), jnp.int32), jnp.zeros((n_dev, TOK), jnp.int32)))[1]
            load.wait()

            @pl.loop(0, tok // block)
            def _(i):
                here = pl.ds(pl.multiple_of(i * block, block), block)
                x = x_buf[here, :].astype(F32)
                mean_sq = jnp.mean(x * x, axis=-1, keepdims=True)
                u = (x * lax.rsqrt(mean_sq + EPS) * gain_row).astype(BF16)
                u_buf[here, :] = u
                logits = lax.dot_general(u, wr_pad[...], (((1,), (1,)), ((), ())), preferred_element_type=F32)
                info = meta[s, here, :]
                l0 = jnp.sum(jnp.where(lane == info[:, 0:1], logits, 0.0), axis=1, keepdims=True)
                l1 = jnp.sum(jnp.where(lane == info[:, 1:2], logits, 0.0), axis=1, keepdims=True)
                top = jnp.maximum(l0, l1)
                e0, e1 = jnp.exp(l0 - top), jnp.exp(l1 - top)
                total = e0 + e1
                probs[s, here, :] = jnp.where(lane == 0, e0 / total, e1 / total)

            @pl.loop(0, 4)
            def _(p):
                row = rows[pl.ds(f * 4 + p, 1), :]
                slot = lax.broadcasted_iota(jnp.int32, (cap, tok), 0)
                onehot[...] = jnp.where(slot == row, 1.0, 0.0).astype(BF16)

                @pl.loop(0, d_model // 256)
                def _(n):
                    cols = pl.ds(pl.multiple_of(n * 256, 256), 256)
                    x_buf[pl.ds(pl.multiple_of(p * cap, cap), cap), cols] = jnp.dot(
                        onehot[...], u_buf[:, cols], preferred_element_type=F32).astype(BF16)

                done = x_buf.at[pl.ds(pl.multiple_of(p * cap, cap), cap)]

                @pl.when(p == j)
                def _():
                    pltpu.make_async_copy(done, x_all.at[pl.ds(owner * cap, cap)], local_sem.at[p]).start()

                @pl.when(p != j)
                def _():
                    pltpu.make_async_copy(done, x_send.at[s, p], local_sem.at[p]).start()

            for p in range(4):
                pltpu.make_async_copy(x_buf.at[pl.ds(p * cap, cap)], x_send.at[s, p], local_sem.at[p]).wait()
            for r in (1, 2, 3):
                x_copy(s, r).start()

        move = pltpu.make_async_copy(base_v, base_s, local_sem.at[0])
        move.start()
        move.wait()

    pl.run_scoped(dispatch, pltpu.VMEM((tok, d_model), BF16), pltpu.VMEM((4 * cap, d_model), BF16), pltpu.VMEM((cap, tok), BF16))

    for s in range(2):
        for r in (1, 2, 3):
            x_copy(s, r).wait_recv()

    bm = 512
    sub = 256

    @pl.loop(0, FF_CHUNKS)
    def _(c):
        gate_copy(c).wait_recv()
        up_copy(c).wait_recv()

        def body(x_own, x_oth, g_own, g_oth, p_own, p_oth, h_ref):
            @pl.loop(0, bm // sub)
            def _(i):
                here = pl.ds(pl.multiple_of(i * sub, sub), sub)
                lhs_own, lhs_oth = x_own[here, :], x_oth[here, :]
                a = jnp.dot(lhs_own, g_own[...], preferred_element_type=F32) + jnp.dot(lhs_oth, g_oth[...], preferred_element_type=F32)
                b = jnp.dot(lhs_own, p_own[...], preferred_element_type=F32) + jnp.dot(lhs_oth, p_oth[...], preferred_element_type=F32)
                h_ref[here, :] = (a * jax.nn.sigmoid(a) * b).astype(BF16)

        pltpu.emit_pipeline(
            body, grid=(n_rows // bm,),
            in_specs=[pl.BlockSpec((bm, half), lambda i: (i, f)), pl.BlockSpec((bm, half), lambda i: (i, 1 - f)),
                      pl.BlockSpec((half, fc), lambda i: (0, c)), pl.BlockSpec((half, fc), lambda i: (0, 0)),
                      pl.BlockSpec((half, fc), lambda i: (0, c)), pl.BlockSpec((half, fc), lambda i: (0, 0))],
            out_specs=[pl.BlockSpec((bm, fc), lambda i: (i, c))],
        )(x_all, x_all, wg.at[f], gate_in.at[c], wu.at[f], up_in.at[c], h_all)

    def project(h_ref, w_ref, o_ref):
        @pl.loop(0, bm // sub)
        def _(i):
            here = pl.ds(pl.multiple_of(i * sub, sub), sub)
            o_ref[here, :] = jnp.dot(h_ref[here, :], w_ref[...], preferred_element_type=F32).astype(BF16)

    def finish(picks, segs, mix, y_buf, window, window_piece):
        side_rows = 4 * WINDOW
        lane = lax.broadcasted_iota(jnp.int32, (1, side_rows), 1)

        def expert_out(phase, q):
            if phase == 0:
                weight, col, chunk = wd.at[f], q, f * HALF_CHUNKS + q
            else:
                down_copy(q).wait_recv()
                weight, col, chunk = down_in.at[q], 0, (1 - f) * HALF_CHUNKS + q
            pltpu.emit_pipeline(
                project, grid=(n_rows // bm,),
                in_specs=[pl.BlockSpec((bm, ff), lambda i: (i, 0)), pl.BlockSpec((ff, dc), lambda i: (0, col))],
                out_specs=[pl.BlockSpec((bm, dc), lambda i: (i, 0))],
            )(h_all, weight, o_all.at[chunk])
            for s in (1, 0):
                for r in (1, 2, 3):
                    back_copy(s, chunk, r).start()

        def fill(s, chunk, cols, buf):
            moves = []
            for r in range(4):
                pj = peer(r)[1]
                owner = (f if s == 0 else 1 - f) * 4 + j
                src = back.at[s, chunk, pl.ds(pj * cap, cap), cols] if r else o_all.at[chunk, pl.ds(owner * cap, cap), cols]
                moves.append(pltpu.make_async_copy(src, buf.at[pl.ds(pj * cap, cap)], local_sem.at[2 + r]))
            return moves

        def take(s, i, buf, win):
            for p in range(4):
                win[p * WINDOW:(p + 1) * WINDOW, :] = buf[pl.ds(base_s[s, f * 4 + p, i] * 16, WINDOW), :]
            picked = jnp.dot(picks[s, i], win[...], preferred_element_type=F32)
            return picked[:TOK], picked[TOK:]

        def relay(half_id, q):
            chunk = half_id * HALF_CHUNKS + q
            for r in (1, 2, 3):
                back_copy(1, chunk, r).wait_recv()
            cols = pl.ds(pl.multiple_of(chunk * dc, PIECE), dc)
            moves = fill(1, chunk, pl.ds(0, dc), segs) + [pltpu.make_async_copy(hid_oth.at[:, cols], mix, local_sem.at[0])]
            for move in moves:
                move.start()
            for move in moves:
                move.wait()

            @pl.loop(0, n_blocks)
            def _(i):
                here = pl.ds(pl.multiple_of(i * TOK, TOK), TOK)
                r0, r1 = take(1, i, segs, window)
                info, p = meta[1, here, :], probs[1, here, :]
                both = (lax.rem(info[:, 0:1], 2) == f) & (lax.rem(info[:, 1:2], 2) == f)
                whole = mix[here, :].astype(F32) + (p[:, 0:1] * r0 + p[:, 1:2] * r1)
                mix[here, :] = jnp.where(both, whole, r0 + r1).astype(BF16)

            moves = [pltpu.make_async_copy(mix.at[:, pl.ds(k * PIECE, PIECE)], y_own.at[chunk * pieces + k], local_sem.at[k]) for k in range(pieces)]
            for move in moves:
                move.start()
            for move in moves:
                move.wait()
            for k in range(pieces):
                y_copy(chunk * pieces + k).start()

        def near_copies(chunk):
            cols = pl.ds(pl.multiple_of(chunk * dc, PIECE), dc)
            return fill(0, chunk, pl.ds(0, dc), segs) + [pltpu.make_async_copy(hid.at[:, cols], mix, local_sem.at[0])]

        def start_near(chunk):
            for r in (1, 2, 3):
                back_copy(0, chunk, r).wait_recv()
            for move in near_copies(chunk):
                move.start()

        def settle(here, r0, r1, k):
            info, p = meta[0, here, :], probs[0, here, :]
            near0, near1 = lax.rem(info[:, 0:1], 2) == f, lax.rem(info[:, 1:2], 2) == f
            cols = slice(k * PIECE, (k + 1) * PIECE)
            far = y_buf[k, here, :].astype(F32)
            c0, c1 = jnp.where(near0, r0, far), jnp.where(near1, r1, far)
            whole = mix[here, cols].astype(F32) + (p[:, 0:1] * c0 + p[:, 1:2] * c1)
            mix[here, cols] = jnp.where(near0 | near1, whole, far).astype(BF16)

        def final(half_id, q):
            chunk = half_id * HALF_CHUNKS + q
            cols = pl.ds(pl.multiple_of(chunk * dc, PIECE), dc)
            start_near(chunk)
            loads = [pltpu.make_async_copy(y_oth.at[chunk * pieces + k], y_buf.at[k], y_sem.at[k]) for k in range(pieces)]
            for k in range(pieces):
                y_copy(chunk * pieces + k).wait_recv()
                loads[k].start()
            for move in near_copies(chunk) + loads:
                move.wait()

            @pl.loop(0, n_blocks)
            def _(i):
                here = pl.ds(pl.multiple_of(i * TOK, TOK), TOK)
                r0, r1 = take(0, i, segs, window)
                for k in range(pieces):
                    settle(here, r0[:, k * PIECE:(k + 1) * PIECE], r1[:, k * PIECE:(k + 1) * PIECE], k)

            store = pltpu.make_async_copy(mix, out.at[:, cols], local_sem.at[0])
            store.start()
            store.wait()

        def final_last():
            chunk = f * HALF_CHUNKS + HALF_CHUNKS - 1
            start_near(chunk)
            for move in near_copies(chunk):
                move.wait()
            stores = []
            for k in range(pieces):
                piece = chunk * pieces + k
                y_copy(piece).wait_recv()
                load = pltpu.make_async_copy(y_oth.at[piece], y_buf.at[k], y_sem.at[k])
                load.start()
                load.wait()

                @pl.loop(0, n_blocks)
                def _(i):
                    here = pl.ds(pl.multiple_of(i * TOK, TOK), TOK)
                    r0, r1 = take(0, i, segs.at[:, pl.ds(k * PIECE, PIECE)], window_piece)
                    settle(here, r0, r1, k)

                stores.append(pltpu.make_async_copy(mix.at[:, pl.ds(k * PIECE, PIECE)],
                                                    out.at[:, pl.ds(pl.multiple_of(piece * PIECE, PIECE), PIECE)], y_sem.at[k]))
                stores[k].start()
            for store in stores:
                store.wait()

        for s in range(2):
            @pl.loop(0, n_blocks)
            def _(i):
                shift = jnp.zeros_like(lane)
                for p in range(4):
                    shift = jnp.where(lane >= p * WINDOW, base_s[s, f * 4 + p, i] * 16 - p * WINDOW, shift)
                row = lane + shift
                info = meta[s, pl.ds(pl.multiple_of(i * TOK, TOK), TOK), :]
                for k in range(2):
                    picks[s, i, k * TOK:(k + 1) * TOK, :] = jnp.where(row == info[:, 2 + k:3 + k], 1.0, 0.0).astype(BF16)

        @pl.loop(0, HALF_CHUNKS)
        def _(q):
            expert_out(0, q)

        @pl.loop(0, HALF_CHUNKS)
        def _(q):
            expert_out(1, q)

            @pl.when(q == 0)
            def _():
                @pl.loop(0, HALF_CHUNKS)
                def _(z):
                    relay(f, z)

        @pl.loop(0, HALF_CHUNKS)
        def _(q):
            relay(1 - f, q)

        @pl.loop(0, 2 * HALF_CHUNKS - 1)
        def _(step):
            final(jnp.where(step < HALF_CHUNKS, 1 - f, f), lax.rem(step, HALF_CHUNKS))

        final_last()

    pl.run_scoped(finish, pltpu.VMEM((2, n_blocks, 2 * TOK, 4 * WINDOW), BF16), pltpu.VMEM((4 * cap, dc), BF16), pltpu.VMEM((tok, dc), BF16),
                  pltpu.VMEM((pieces, tok, PIECE), BF16),
                  pltpu.VMEM((4 * WINDOW, dc), BF16), pltpu.VMEM((4 * WINDOW, PIECE), BF16))

    ids_copy().wait_send()
    hid_copy().wait_send()
    for c in range(FF_CHUNKS):
        gate_copy(c).wait_send()
        up_copy(c).wait_send()
    for q in range(HALF_CHUNKS):
        down_copy(q).wait_send()
    for s in range(2):
        for r in (1, 2, 3):
            x_copy(s, r).wait_send()

    @pl.loop(0, chunks)
    def _(chunk):
        for s in range(2):
            for r in (1, 2, 3):
                back_copy(s, chunk, r).wait_send()
        for k in range(pieces):
            y_copy(chunk * pieces + k).wait_send()


def local_block(hidden, norm_gain, w_router, w_gate, w_up, w_down, top2_ids):
    tok, d_model = hidden.shape
    num_experts = w_router.shape[1]
    half, ff = w_gate.shape[1:]
    cap = (5 * tok + 2 * num_experts - 1) // (2 * num_experts)
    fc, dc = ff // FF_CHUNKS, half // HALF_CHUNKS
    n_rows = num_experts * cap
    shape = lambda *s: jax.ShapeDtypeStruct(s, BF16)
    dma = pltpu.SemaphoreType.DMA
    results = pl.pallas_call(
        functools.partial(moe_kernel, cap),
        out_shape=[shape(tok, d_model), shape(tok, d_model),
                   shape(FF_CHUNKS, half, fc), shape(FF_CHUNKS, half, fc), shape(HALF_CHUNKS, ff, dc),
                   shape(2, 4, cap, d_model), shape(n_rows, d_model), shape(n_rows, ff),
                   shape(2 * HALF_CHUNKS, n_rows, dc), shape(2, 2 * HALF_CHUNKS, 4 * cap, dc),
                   shape(d_model // PIECE, tok, PIECE), shape(d_model // PIECE, tok, PIECE)],
        in_specs=[ANY, VMEM, VMEM, VMEM, ANY, ANY, ANY],
        out_specs=[ANY] * 12,
        scratch_shapes=[
            pltpu.VMEM((num_experts, tok), jnp.int32), pltpu.VMEM((2, tok), jnp.int32),
            pltpu.VMEM((2, tok, 128), jnp.int32), pltpu.VMEM((2, tok, 128), F32), pltpu.VMEM((128, d_model), BF16),
            pltpu.VMEM((2, num_experts, TOK), jnp.int32), pltpu.SMEM((2, num_experts, TOK), jnp.int32),
            dma((6,)), dma((2, FF_CHUNKS)), dma((2, FF_CHUNKS)), dma((HALF_CHUNKS,)), dma((HALF_CHUNKS,)),
            dma((2,)), dma((2,)), dma((2, 4)), dma((2, 4)),
            dma((4 * HALF_CHUNKS, 4)), dma((4 * HALF_CHUNKS, 4)), dma((d_model // PIECE,)), dma((d_model // PIECE,)), dma((half // HALF_CHUNKS // PIECE,))],
        compiler_params=pltpu.CompilerParams(collective_id=0, has_side_effects=True, vmem_limit_bytes=62 * 1024 * 1024),
    )(hidden, norm_gain, w_router.T, top2_ids.T, w_gate, w_up, w_down)
    return results[0]


def solution(mesh):
    tok_spec = P(('dp', 'fsdp', 'ep'), None)
    in_specs = (tok_spec, P(None), P(None, None), P('ep', 'fsdp', None), P('ep', 'fsdp', None), P('ep', None, 'fsdp'), tok_spec)
    return jax.shard_map(local_block, mesh=mesh, in_specs=in_specs, out_specs=tok_spec, check_vma=False)
```

```python
import functools

import jax
import jax.numpy as jnp
from jax import lax
from jax.experimental import pallas as pl
from jax.experimental.pallas import tpu as pltpu
from jax.sharding import PartitionSpec as P

EPS = 1e-5
MESH = pl.DeviceIdType.MESH
ANY = pl.BlockSpec(memory_space=pl.ANY)
VMEM = pl.BlockSpec(memory_space=pltpu.VMEM)
F32 = jnp.float32
BF16 = jnp.bfloat16
FF_CHUNKS = 5
HALF_CHUNKS = 3
PIECE = 128
PARTS = 2
TOK = 128
WINDOW = TOK + 16


def moe_kernel(cap, hid, gain, wr, ids, wg, wu, wd,
               out, hid_oth, gate_in, up_in, down_in, x_send, x_all, h_all, o_all, back, y_own, y_oth,
               rows, ids_oth, meta, probs, wr_pad, base_v, base_s, local_sem, w_send, w_recv, d_send, d_recv,
               u_send, u_recv, x_ssem, x_rsem, b_send, b_recv, y_send, y_recv, y_sem):
    tok, d_model = hid.shape
    half = d_model // 2
    ff = wg.shape[2]
    fc = ff // FF_CHUNKS
    dc = half // HALF_CHUNKS
    n_dev = 8
    pieces = dc // PIECE
    n_rows = n_dev * cap
    chunks = 2 * HALF_CHUNKS
    n_blocks = tok // TOK
    f = lax.axis_index('fsdp')
    j = lax.axis_index('ep')
    me = f * 4 + j
    j_low, j_high = lax.rem(j, 2), lax.div(j, 2)

    def peer(r):
        pf = 1 - f if r // 4 else f
        pj = (1 - j_low if r & 1 else j_low) + 2 * (1 - j_high if r & 2 else j_high)
        return pf, pj

    def remote(src, dst, ssem, rsem, r):
        pf, pj = peer(r)
        return pltpu.make_async_remote_copy(src_ref=src, dst_ref=dst, send_sem=ssem, recv_sem=rsem,
                                            device_id={'fsdp': pf, 'ep': pj}, device_id_type=MESH)

    def gate_copy(c):
        return remote(wg.at[1 - f, :, pl.ds(c * fc, fc)], gate_in.at[c], w_send.at[0, c], w_recv.at[0, c], 4)

    def up_copy(c):
        return remote(wu.at[1 - f, :, pl.ds(c * fc, fc)], up_in.at[c], w_send.at[1, c], w_recv.at[1, c], 4)

    def down_copy(q):
        return remote(wd.at[1 - f, :, pl.ds(q * dc, dc)], down_in.at[q], d_send.at[q], d_recv.at[q], 4)

    def ids_copy():
        return remote(ids, ids_oth, u_send.at[0], u_recv.at[0], 4)

    def hid_copy():
        return remote(hid, hid_oth, u_send.at[1], u_recv.at[1], 4)

    def x_copy(s, r):
        pf, pj = peer(r)
        owner = me if s == 0 else (1 - f) * 4 + j
        return remote(x_send.at[s, pj], x_all.at[pl.ds(owner * cap, cap)], x_ssem.at[s, r], x_rsem.at[s, r], r)

    def back_copy(s, chunk, r):
        pf, pj = peer(r)
        owner = (f if s == 0 else 1 - f) * 4 + pj
        return remote(o_all.at[chunk, pl.ds(owner * cap, cap)], back.at[s, chunk, pl.ds(j * cap, cap)],
                      b_send.at[s * chunks + chunk, r], b_recv.at[s * chunks + chunk, r], r)

    def y_copy(piece, part):
        here = pl.ds(part * (tok // PARTS), tok // PARTS)
        return remote(y_own.at[piece, here], y_oth.at[piece, here], y_send.at[piece, part], y_recv.at[piece, part], 4)

    barrier = pltpu.get_barrier_semaphore()
    for r in range(1, n_dev):
        pf, pj = peer(r)
        pl.semaphore_signal(barrier, inc=1, device_id={'fsdp': pf, 'ep': pj}, device_id_type=MESH)
    pl.semaphore_wait(barrier, n_dev - 1)

    ids_copy().start()
    hid_copy().start()
    for c in range(FF_CHUNKS):
        gate_copy(c).start()
        up_copy(c).start()
    for q in range(HALF_CHUNKS):
        down_copy(q).start()

    wr_pad[...] = jnp.zeros_like(wr_pad)
    wr_pad[0:n_dev, :] = wr[...]
    tri = (lax.broadcasted_iota(jnp.int32, (TOK, TOK), 0) < lax.broadcasted_iota(jnp.int32, (TOK, TOK), 1)).astype(F32).astype(BF16)
    spot = lax.broadcasted_iota(jnp.int32, (n_dev, TOK), 0)
    column = lax.broadcasted_iota(jnp.int32, (n_dev, TOK), 1)
    line = lax.broadcasted_iota(jnp.int32, (TOK, TOK), 0)

    def route(s, ids_ref, blk, carry):
        count, bases = carry
        here = pl.ds(pl.multiple_of(blk * TOK, TOK), TOK)
        id0, id1 = ids_ref[0:1, here], ids_ref[1:2, here]
        place0 = lax.rem(id0, 2) * 4 + lax.div(id0, 2)
        place1 = lax.rem(id1, 2) * 4 + lax.div(id1, 2)
        chosen = (spot == place0) | (spot == place1)
        before = jnp.dot(jnp.where(chosen, 1.0, 0.0).astype(BF16), tri, preferred_element_type=F32)
        position = before.astype(jnp.int32) + count
        kept = jnp.where(chosen & (position < cap), position, -1)
        rows[:, here] = kept
        mine = (spot >= f * 4) & (spot < f * 4 + 4)
        flat = jnp.where(mine & (kept >= 0), kept + (spot - f * 4) * cap, -1)
        slot0 = jnp.sum(jnp.where(spot == place0, flat, 0), axis=0, keepdims=True)
        slot1 = jnp.sum(jnp.where(spot == place1, flat, 0), axis=0, keepdims=True)
        stacked = jnp.where(line == 0, id0, jnp.where(line == 1, id1, jnp.where(line == 2, slot0, slot1)))
        meta[s, here, :] = stacked.astype(F32).T.astype(jnp.int32)
        start = jnp.minimum(lax.div(count, 16), (cap - WINDOW) // 16)
        bases = jnp.where(column == blk, start + lax.rem(spot, 4) * (cap // 16), bases)
        return count + jnp.sum(jnp.where(chosen, 1, 0), axis=1, keepdims=True), bases

    def dispatch(u_buf, x_buf, onehot):
        block = 128
        gain_row = gain[...].astype(F32)[None, :]
        lane = lax.broadcasted_iota(jnp.int32, (block, 128), 1)

        for s in range(2):
            owner = me if s == 0 else (1 - f) * 4 + j
            if s == 1:
                ids_copy().wait_recv()
                hid_copy().wait_recv()
            load = pltpu.make_async_copy(hid if s == 0 else hid_oth, x_buf.at[pl.ds(0, tok)], local_sem.at[0])
            load.start()
            base_v[s] = lax.fori_loop(0, n_blocks, functools.partial(route, s, ids if s == 0 else ids_oth),
                                      (jnp.zeros((n_dev, 1), jnp.int32), jnp.zeros((n_dev, TOK), jnp.int32)))[1]
            load.wait()

            @pl.loop(0, tok // block)
            def _(i):
                here = pl.ds(pl.multiple_of(i * block, block), block)
                x = x_buf[here, :].astype(F32)
                mean_sq = jnp.mean(x * x, axis=-1, keepdims=True)
                u = (x * lax.rsqrt(mean_sq + EPS) * gain_row).astype(BF16)
                u_buf[here, :] = u
                logits = lax.dot_general(u, wr_pad[...], (((1,), (1,)), ((), ())), preferred_element_type=F32)
                info = meta[s, here, :]
                l0 = jnp.sum(jnp.where(lane == info[:, 0:1], logits, 0.0), axis=1, keepdims=True)
                l1 = jnp.sum(jnp.where(lane == info[:, 1:2], logits, 0.0), axis=1, keepdims=True)
                top = jnp.maximum(l0, l1)
                e0, e1 = jnp.exp(l0 - top), jnp.exp(l1 - top)
                total = e0 + e1
                probs[s, here, :] = jnp.where(lane == 0, e0 / total, e1 / total)

            @pl.loop(0, 4)
            def _(p):
                row = rows[pl.ds(f * 4 + p, 1), :]
                slot = lax.broadcasted_iota(jnp.int32, (cap, tok), 0)
                onehot[...] = jnp.where(slot == row, 1.0, 0.0).astype(BF16)

                @pl.loop(0, d_model // 256)
                def _(n):
                    cols = pl.ds(pl.multiple_of(n * 256, 256), 256)
                    x_buf[pl.ds(pl.multiple_of(p * cap, cap), cap), cols] = jnp.dot(
                        onehot[...], u_buf[:, cols], preferred_element_type=F32).astype(BF16)

                done = x_buf.at[pl.ds(pl.multiple_of(p * cap, cap), cap)]

                @pl.when(p == j)
                def _():
                    pltpu.make_async_copy(done, x_all.at[pl.ds(owner * cap, cap)], local_sem.at[p]).start()

                @pl.when(p != j)
                def _():
                    pltpu.make_async_copy(done, x_send.at[s, p], local_sem.at[p]).start()

            for p in range(4):
                pltpu.make_async_copy(x_buf.at[pl.ds(p * cap, cap)], x_send.at[s, p], local_sem.at[p]).wait()
            for r in (1, 2, 3):
                x_copy(s, r).start()

        move = pltpu.make_async_copy(base_v, base_s, local_sem.at[0])
        move.start()
        move.wait()

    pl.run_scoped(dispatch, pltpu.VMEM((tok, d_model), BF16), pltpu.VMEM((4 * cap, d_model), BF16), pltpu.VMEM((cap, tok), BF16))

    for s in range(2):
        for r in (1, 2, 3):
            x_copy(s, r).wait_recv()

    bm = 512
    sub = 256

    @pl.loop(0, FF_CHUNKS)
    def _(c):
        gate_copy(c).wait_recv()
        up_copy(c).wait_recv()

        def body(x_own, x_oth, g_own, g_oth, p_own, p_oth, h_ref):
            @pl.loop(0, bm // sub)
            def _(i):
                here = pl.ds(pl.multiple_of(i * sub, sub), sub)
                lhs_own, lhs_oth = x_own[here, :], x_oth[here, :]
                a = jnp.dot(lhs_own, g_own[...], preferred_element_type=F32) + jnp.dot(lhs_oth, g_oth[...], preferred_element_type=F32)
                b = jnp.dot(lhs_own, p_own[...], preferred_element_type=F32) + jnp.dot(lhs_oth, p_oth[...], preferred_element_type=F32)
                h_ref[here, :] = (a * jax.nn.sigmoid(a) * b).astype(BF16)

        pltpu.emit_pipeline(
            body, grid=(n_rows // bm,),
            in_specs=[pl.BlockSpec((bm, half), lambda i: (i, f)), pl.BlockSpec((bm, half), lambda i: (i, 1 - f)),
                      pl.BlockSpec((half, fc), lambda i: (0, c)), pl.BlockSpec((half, fc), lambda i: (0, 0)),
                      pl.BlockSpec((half, fc), lambda i: (0, c)), pl.BlockSpec((half, fc), lambda i: (0, 0))],
            out_specs=[pl.BlockSpec((bm, fc), lambda i: (i, c))],
        )(x_all, x_all, wg.at[f], gate_in.at[c], wu.at[f], up_in.at[c], h_all)

    def project(h_ref, w_ref, o_ref):
        @pl.loop(0, bm // sub)
        def _(i):
            here = pl.ds(pl.multiple_of(i * sub, sub), sub)
            o_ref[here, :] = jnp.dot(h_ref[here, :], w_ref[...], preferred_element_type=F32).astype(BF16)

    def finish(picks, segs, mix, y_buf, window, near):
        side_rows = 4 * WINDOW
        lane = lax.broadcasted_iota(jnp.int32, (1, side_rows), 1)

        def expert_out(phase, q):
            if phase == 0:
                weight, col, chunk = wd.at[f], q, f * HALF_CHUNKS + q
            else:
                down_copy(q).wait_recv()
                weight, col, chunk = down_in.at[q], 0, (1 - f) * HALF_CHUNKS + q
            pltpu.emit_pipeline(
                project, grid=(n_rows // bm,),
                in_specs=[pl.BlockSpec((bm, ff), lambda i: (i, 0)), pl.BlockSpec((ff, dc), lambda i: (0, col))],
                out_specs=[pl.BlockSpec((bm, dc), lambda i: (i, 0))],
            )(h_all, weight, o_all.at[chunk])
            for s in (1, 0):
                for r in (1, 2, 3):
                    back_copy(s, chunk, r).start()

        def fill(s, chunk, cols, buf):
            moves = []
            for r in range(4):
                pj = peer(r)[1]
                owner = (f if s == 0 else 1 - f) * 4 + j
                src = back.at[s, chunk, pl.ds(pj * cap, cap), cols] if r else o_all.at[chunk, pl.ds(owner * cap, cap), cols]
                moves.append(pltpu.make_async_copy(src, buf.at[pl.ds(pj * cap, cap)], local_sem.at[2 + r]))
            return moves

        def take(s, i, buf, win):
            for p in range(4):
                win[p * WINDOW:(p + 1) * WINDOW, :] = buf[pl.ds(base_s[s, f * 4 + p, i] * 16, WINDOW), :]
            picked = jnp.dot(picks[s, i], win[...], preferred_element_type=F32)
            return picked[:TOK], picked[TOK:]

        def relay(half_id, q):
            chunk = half_id * HALF_CHUNKS + q
            for r in (1, 2, 3):
                back_copy(1, chunk, r).wait_recv()
            cols = pl.ds(pl.multiple_of(chunk * dc, PIECE), dc)
            moves = fill(1, chunk, pl.ds(0, dc), segs) + [pltpu.make_async_copy(hid_oth.at[:, cols], mix, local_sem.at[0])]
            for move in moves:
                move.start()
            for move in moves:
                move.wait()

            @pl.loop(0, n_blocks)
            def _(i):
                here = pl.ds(pl.multiple_of(i * TOK, TOK), TOK)
                r0, r1 = take(1, i, segs, window)
                info, p = meta[1, here, :], probs[1, here, :]
                both = (lax.rem(info[:, 0:1], 2) == f) & (lax.rem(info[:, 1:2], 2) == f)
                whole = mix[here, :].astype(F32) + (p[:, 0:1] * r0 + p[:, 1:2] * r1)
                mix[here, :] = jnp.where(both, whole, r0 + r1).astype(BF16)

            moves = [pltpu.make_async_copy(mix.at[:, pl.ds(k * PIECE, PIECE)], y_own.at[chunk * pieces + k], local_sem.at[k]) for k in range(pieces)]
            for move in moves:
                move.start()
            for move in moves:
                move.wait()
            for k in range(pieces):
                for part in range(PARTS):
                    y_copy(chunk * pieces + k, part).start()

        def near_copies(chunk):
            cols = pl.ds(pl.multiple_of(chunk * dc, PIECE), dc)
            return fill(0, chunk, pl.ds(0, dc), segs) + [pltpu.make_async_copy(hid.at[:, cols], mix, local_sem.at[0])]

        def start_near(chunk):
            for r in (1, 2, 3):
                back_copy(0, chunk, r).wait_recv()
            for move in near_copies(chunk):
                move.start()

        def settle(here, r0, r1, k):
            info, p = meta[0, here, :], probs[0, here, :]
            near0, near1 = lax.rem(info[:, 0:1], 2) == f, lax.rem(info[:, 1:2], 2) == f
            cols = slice(k * PIECE, (k + 1) * PIECE)
            far = y_buf[k, here, :].astype(F32)
            c0, c1 = jnp.where(near0, r0, far), jnp.where(near1, r1, far)
            whole = mix[here, cols].astype(F32) + (p[:, 0:1] * c0 + p[:, 1:2] * c1)
            mix[here, cols] = jnp.where(near0 | near1, whole, far).astype(BF16)

        def final(half_id, q):
            chunk = half_id * HALF_CHUNKS + q
            cols = pl.ds(pl.multiple_of(chunk * dc, PIECE), dc)
            start_near(chunk)
            loads = [pltpu.make_async_copy(y_oth.at[chunk * pieces + k], y_buf.at[k], y_sem.at[k, 0]) for k in range(pieces)]
            for k in range(pieces):
                for part in range(PARTS):
                    y_copy(chunk * pieces + k, part).wait_recv()
                loads[k].start()
            for move in near_copies(chunk) + loads:
                move.wait()

            @pl.loop(0, n_blocks)
            def _(i):
                here = pl.ds(pl.multiple_of(i * TOK, TOK), TOK)
                r0, r1 = take(0, i, segs, window)
                for k in range(pieces):
                    settle(here, r0[:, k * PIECE:(k + 1) * PIECE], r1[:, k * PIECE:(k + 1) * PIECE], k)

            store = pltpu.make_async_copy(mix, out.at[:, cols], local_sem.at[0])
            store.start()
            store.wait()

        def final_last():
            chunk = f * HALF_CHUNKS + HALF_CHUNKS - 1
            start_near(chunk)
            for move in near_copies(chunk):
                move.wait()

            @pl.loop(0, n_blocks)
            def _(i):
                here = pl.ds(pl.multiple_of(i * TOK, TOK), TOK)
                r0, r1 = take(0, i, segs, window)
                info, p = meta[0, here, :], probs[0, here, :]
                near0, near1 = lax.rem(info[:, 0:1], 2) == f, lax.rem(info[:, 1:2], 2) == f
                near[here, :] = p[:, 0:1] * jnp.where(near0, r0, 0.0) + p[:, 1:2] * jnp.where(near1, r1, 0.0)

            stores = []
            part_rows = tok // PARTS
            for k in range(pieces):
                for part in range(PARTS):
                    piece = chunk * pieces + k
                    rows_here = pl.ds(part * part_rows, part_rows)
                    y_copy(piece, part).wait_recv()
                    load = pltpu.make_async_copy(y_oth.at[piece, rows_here], y_buf.at[k, rows_here], y_sem.at[k, part])
                    load.start()
                    load.wait()
                    cols = slice(k * PIECE, (k + 1) * PIECE)

                    @pl.loop(part * (n_blocks // PARTS), (part + 1) * (n_blocks // PARTS))
                    def _(i):
                        here = pl.ds(pl.multiple_of(i * TOK, TOK), TOK)
                        info, p = meta[0, here, :], probs[0, here, :]
                        near0, near1 = lax.rem(info[:, 0:1], 2) == f, lax.rem(info[:, 1:2], 2) == f
                        p_far = jnp.where(near0, jnp.where(near1, 0.0, p[:, 1:2]), p[:, 0:1])
                        far = y_buf[k, here, :].astype(F32)
                        whole = mix[here, cols].astype(F32) + (near[here, cols] + p_far * far)
                        mix[here, cols] = jnp.where(near0 | near1, whole, far).astype(BF16)

                    store = pltpu.make_async_copy(mix.at[rows_here, pl.ds(k * PIECE, PIECE)],
                                                  out.at[rows_here, pl.ds(pl.multiple_of(piece * PIECE, PIECE), PIECE)], y_sem.at[k, part])
                    store.start()
                    stores.append(store)
            for store in stores:
                store.wait()

        for s in range(2):
            @pl.loop(0, n_blocks)
            def _(i):
                shift = jnp.zeros_like(lane)
                for p in range(4):
                    shift = jnp.where(lane >= p * WINDOW, base_s[s, f * 4 + p, i] * 16 - p * WINDOW, shift)
                row = lane + shift
                info = meta[s, pl.ds(pl.multiple_of(i * TOK, TOK), TOK), :]
                for k in range(2):
                    picks[s, i, k * TOK:(k + 1) * TOK, :] = jnp.where(row == info[:, 2 + k:3 + k], 1.0, 0.0).astype(BF16)

        @pl.loop(0, HALF_CHUNKS)
        def _(q):
            expert_out(0, q)

        @pl.loop(0, HALF_CHUNKS)
        def _(q):
            expert_out(1, q)

            @pl.when(q == 0)
            def _():
                @pl.loop(0, HALF_CHUNKS)
                def _(z):
                    relay(f, z)

        @pl.loop(0, HALF_CHUNKS)
        def _(q):
            relay(1 - f, q)

        @pl.loop(0, 2 * HALF_CHUNKS - 1)
        def _(step):
            final(jnp.where(step < HALF_CHUNKS, 1 - f, f), lax.rem(step, HALF_CHUNKS))

        final_last()

    pl.run_scoped(finish, pltpu.VMEM((2, n_blocks, 2 * TOK, 4 * WINDOW), BF16), pltpu.VMEM((4 * cap, dc), BF16), pltpu.VMEM((tok, dc), BF16),
                  pltpu.VMEM((pieces, tok, PIECE), BF16),
                  pltpu.VMEM((4 * WINDOW, dc), BF16), pltpu.VMEM((tok, dc), F32))

    ids_copy().wait_send()
    hid_copy().wait_send()
    for c in range(FF_CHUNKS):
        gate_copy(c).wait_send()
        up_copy(c).wait_send()
    for q in range(HALF_CHUNKS):
        down_copy(q).wait_send()
    for s in range(2):
        for r in (1, 2, 3):
            x_copy(s, r).wait_send()

    @pl.loop(0, chunks)
    def _(chunk):
        for s in range(2):
            for r in (1, 2, 3):
                back_copy(s, chunk, r).wait_send()
        for k in range(pieces):
            for part in range(PARTS):
                y_copy(chunk * pieces + k, part).wait_send()


def local_block(hidden, norm_gain, w_router, w_gate, w_up, w_down, top2_ids):
    tok, d_model = hidden.shape
    num_experts = w_router.shape[1]
    half, ff = w_gate.shape[1:]
    cap = (5 * tok + 2 * num_experts - 1) // (2 * num_experts)
    fc, dc = ff // FF_CHUNKS, half // HALF_CHUNKS
    n_rows = num_experts * cap
    shape = lambda *s: jax.ShapeDtypeStruct(s, BF16)
    dma = pltpu.SemaphoreType.DMA
    results = pl.pallas_call(
        functools.partial(moe_kernel, cap),
        out_shape=[shape(tok, d_model), shape(tok, d_model),
                   shape(FF_CHUNKS, half, fc), shape(FF_CHUNKS, half, fc), shape(HALF_CHUNKS, ff, dc),
                   shape(2, 4, cap, d_model), shape(n_rows, d_model), shape(n_rows, ff),
                   shape(2 * HALF_CHUNKS, n_rows, dc), shape(2, 2 * HALF_CHUNKS, 4 * cap, dc),
                   shape(d_model // PIECE, tok, PIECE), shape(d_model // PIECE, tok, PIECE)],
        in_specs=[ANY, VMEM, VMEM, VMEM, ANY, ANY, ANY],
        out_specs=[ANY] * 12,
        scratch_shapes=[
            pltpu.VMEM((num_experts, tok), jnp.int32), pltpu.VMEM((2, tok), jnp.int32),
            pltpu.VMEM((2, tok, 128), jnp.int32), pltpu.VMEM((2, tok, 128), F32), pltpu.VMEM((128, d_model), BF16),
            pltpu.VMEM((2, num_experts, TOK), jnp.int32), pltpu.SMEM((2, num_experts, TOK), jnp.int32),
            dma((6,)), dma((2, FF_CHUNKS)), dma((2, FF_CHUNKS)), dma((HALF_CHUNKS,)), dma((HALF_CHUNKS,)),
            dma((2,)), dma((2,)), dma((2, 4)), dma((2, 4)),
            dma((4 * HALF_CHUNKS, 4)), dma((4 * HALF_CHUNKS, 4)), dma((d_model // PIECE, PARTS)), dma((d_model // PIECE, PARTS)), dma((half // HALF_CHUNKS // PIECE, PARTS))],
        compiler_params=pltpu.CompilerParams(collective_id=0, has_side_effects=True, vmem_limit_bytes=62 * 1024 * 1024),
    )(hidden, norm_gain, w_router.T, top2_ids.T, w_gate, w_up, w_down)
    return results[0]


def solution(mesh):
    tok_spec = P(('dp', 'fsdp', 'ep'), None)
    in_specs = (tok_spec, P(None), P(None, None), P('ep', 'fsdp', None), P('ep', 'fsdp', None), P('ep', None, 'fsdp'), tok_spec)
    return jax.shard_map(local_block, mesh=mesh, in_specs=in_specs, out_specs=tok_spec, check_vma=False)
```
